32 devices in a mesh: dp: 1 (over z), tp: 4 (over y), ep: 8 (over x, core).
Axes of the slice: x: 4, y: 4, z: 1, core: 2. Of those that a mesh axis runs over, the one named last changes fastest.
The devices are a block of a 4x4x8 slice.
Arguments:
- x_in: bfloat16 [2048, 1536], P(('dp', 'ep', 'tp'))
- norm_gain: bfloat16 [1536], replicated
- w_router: bfloat16 [1536, 40], replicated
- expert_idx: int32 [2048, 8], P(('dp', 'ep', 'tp'))
- w_gate: bfloat16 [40, 1536, 512], P('ep', None, 'tp')
- w_up: bfloat16 [40, 1536, 512], P('ep', None, 'tp')
- w_down: bfloat16 [40, 512, 1536], P('ep', 'tp')
- out_bias: bfloat16 [1536], replicated
- dy_out: bfloat16 [2048, 1536], P(('dp', 'ep', 'tp'))
Outputs:
- output 1: bfloat16 [2048, 1536], P(('dp', 'ep', 'tp'))
- output 2: bfloat16 [2048, 1536], P(('dp', 'ep', 'tp'))
- output 3: float32 [1536], P('dp')
- output 4: float32 [1536, 40], P('dp')
- output 5: float32 [40, 1536, 512], P(('dp', 'ep'), None, 'tp')
- output 6: float32 [40, 1536, 512], P(('dp', 'ep'), None, 'tp')
- output 7: float32 [40, 512, 1536], P(('dp', 'ep'), 'tp')
- output 8: float32 [1536], P('dp')
All inputs are finite; a program needn't handle non-finite values.
Results may differ from the reference program's by a relative error of at most 0.0116395.
Values are sent between devices in bfloat16 or wider.
A program may use at most 768 MiB of HBM per device.

```python
import jax
import jax.numpy as jnp
from jax import lax

TOK = 64
D = 1536
FF = 512
EXPERTS = 40
TOP = 8
EP_DEVS = 8
TP_DEVS = 4
CAP = 26
EPS = 1e-6


def permute_tokens(perm_key):
    return jax.random.permutation(perm_key, TOK)


def draw_routing(route_key):
    n_src = EP_DEVS * TP_DEVS
    key_heavy, key_weight, key_perm = jax.random.split(route_key, 3)
    expert_row = jnp.arange(EXPERTS)[None, :]
    heavy = jax.random.randint(key_heavy, (n_src, 1), 0, EXPERTS)
    is_heavy = expert_row == heavy
    weights = jnp.where(is_heavy, 0, jax.random.randint(key_weight, (n_src, EXPERTS), 2, 5))
    rest = TOK * TOP - CAP
    share = rest * weights // jnp.sum(weights, axis=1, keepdims=True)
    left_over = rest - jnp.sum(share, axis=1, keepdims=True)
    light_rank = jnp.cumsum(jnp.where(is_heavy, 0, 1), axis=1) - 1
    extra = jnp.where(jnp.logical_and(jnp.logical_not(is_heavy), light_rank < left_over), 1, 0)
    counts = jnp.where(is_heavy, CAP, share + extra)
    ends = jnp.cumsum(counts, axis=1)
    position = jnp.arange(TOP)[None, :] * TOK + jnp.arange(TOK)[:, None]
    choice = jnp.sum((position[None, :, :, None] >= ends[:, None, None, :]).astype(jnp.int32), axis=-1)
    perms = jax.vmap(permute_tokens)(jax.random.split(key_perm, n_src))
    choice = jnp.take_along_axis(choice, perms[:, :, None], axis=1)
    return choice.reshape(n_src * TOK, TOP).astype(jnp.int32)


def setup_inputs(seed: int = 0, part: int = 0) -> dict:
    part_key = jax.random.fold_in(jax.random.key(seed), part)
    key_x, key_dy, key_route = jax.random.split(part_key, 3)
    key_g, key_r, key_wg, key_wu, key_wd, key_b = jax.random.split(jax.random.key(seed + 1), 6)
    n_rows = EP_DEVS * TP_DEVS * TOK
    x_in = jax.random.normal(key_x, (n_rows, D), jnp.float32).astype(jnp.bfloat16)
    norm_gain = (1.0 + 0.3 * jax.random.normal(key_g, (D,), jnp.float32)).astype(jnp.bfloat16)
    w_router = (2.0 * D ** -0.5 * jax.random.normal(key_r, (D, EXPERTS), jnp.float32)).astype(jnp.bfloat16)
    w_gate = (D ** -0.5 * jax.random.normal(key_wg, (EXPERTS, D, FF), jnp.float32)).astype(jnp.bfloat16)
    w_up = (D ** -0.5 * jax.random.normal(key_wu, (EXPERTS, D, FF), jnp.float32)).astype(jnp.bfloat16)
    w_down = (1.5 * FF ** -0.5 * jax.random.normal(key_wd, (EXPERTS, FF, D), jnp.float32)).astype(jnp.bfloat16)
    out_bias = (0.5 * jax.random.normal(key_b, (D,), jnp.float32)).astype(jnp.bfloat16)
    dy_out = jax.random.normal(key_dy, (n_rows, D), jnp.float32).astype(jnp.bfloat16)
    expert_idx = draw_routing(key_route)
    return {"x_in": x_in, "norm_gain": norm_gain, "w_router": w_router, "expert_idx": expert_idx, "w_gate": w_gate, "w_up": w_up, "w_down": w_down, "out_bias": out_bias, "dy_out": dy_out}


def to_bf16(values):
    return values + lax.stop_gradient(values.astype(jnp.bfloat16).astype(jnp.float32) - values)


def reference(x_in, norm_gain, w_router, expert_idx, w_gate, w_up, w_down, out_bias, dy_out):
    n_rows = x_in.shape[0]
    rows_max = EP_DEVS * TP_DEVS * CAP
    flat_ids = expert_idx.reshape(-1)
    order = jnp.argsort(flat_ids, stable=True)
    counts = jnp.sum((flat_ids[:, None] == jnp.arange(EXPERTS)[None, :]).astype(jnp.int32), axis=0)
    starts = jnp.cumsum(counts) - counts
    slot_rank = jnp.arange(rows_max)[None, :]
    slot_tok = order[jnp.minimum(starts[:, None] + slot_rank, n_rows * TOP - 1)] // TOP
    slot_ok = slot_rank < counts[:, None]
    copy_pos = (flat_ids * rows_max + jnp.argsort(order) - starts[flat_ids]).reshape(n_rows, TOP)

    def forward(x_f32, gain, router, gate_w, up_w, down_w, bias):
        inv_rms = lax.rsqrt(jnp.mean(x_f32 * x_f32, axis=-1, keepdims=True) + EPS)
        hidden = to_bf16(x_f32 * inv_rms * gain)
        logits = jnp.dot(hidden, router, preferred_element_type=jnp.float32)
        gates = jax.nn.softmax(jnp.take_along_axis(logits, expert_idx, axis=1), axis=-1)

        def one_expert(operands):
            gate_e, up_e, down_e, tok_e, ok_e = operands
            rows_in = jnp.where(ok_e[:, None], hidden[tok_e], 0.0)
            gate_pre = jnp.dot(rows_in, gate_e, preferred_element_type=jnp.float32)
            up_pre = jnp.dot(rows_in, up_e, preferred_element_type=jnp.float32)
            hidden_act = to_bf16(jax.nn.silu(gate_pre) * up_pre)
            return to_bf16(jnp.dot(hidden_act, down_e, preferred_element_type=jnp.float32))

        y_slots = lax.map(jax.checkpoint(one_expert), (gate_w, up_w, down_w, slot_tok, slot_ok))
        y_copy = y_slots.reshape(EXPERTS * rows_max, D)[copy_pos]
        return x_f32 + jnp.sum(gates[:, :, None] * y_copy, axis=1) + bias

    y_f32, pullback = jax.vjp(forward, x_in.astype(jnp.float32), norm_gain.astype(jnp.float32), w_router.astype(jnp.float32), w_gate.astype(jnp.float32), w_up.astype(jnp.float32), w_down.astype(jnp.float32), out_bias.astype(jnp.float32))
    cotangents = pullback(dy_out.astype(jnp.float32))
    return (y_f32.astype(jnp.bfloat16), cotangents[0].astype(jnp.bfloat16), cotangents[1], cotangents[2], cotangents[3], cotangents[4], cotangents[5], cotangents[6])
```

```python
import jax
import jax.numpy as jnp
from jax import lax
from jax.sharding import PartitionSpec as P

EPS = 1e-6


def solution(mesh):
    tok_spec = P(("dp", "ep", "tp"), None)
    wide_spec = P("ep", None, "tp")
    down_spec = P("ep", "tp", None)
    grad_wide = P(("dp", "ep"), None, "tp")
    grad_down = P(("dp", "ep"), "tp", None)
    group = ("ep", "tp")

    def device_step(x_in, norm_gain, w_router, expert_idx, w_gate, w_up, w_down, out_bias, dy_out):
        n_exp = w_router.shape[1]
        local_exp = w_gate.shape[0]
        x_f32 = x_in.astype(jnp.float32)
        inv_rms = lax.rsqrt(jnp.mean(x_f32 * x_f32, axis=-1, keepdims=True) + EPS)
        normed = x_f32 * inv_rms
        gain_f32 = norm_gain.astype(jnp.float32)
        hidden = (normed * gain_f32).astype(jnp.bfloat16)
        logits = jnp.dot(hidden, w_router, preferred_element_type=jnp.float32)
        chosen = expert_idx[:, :, None] == jnp.arange(n_exp)[None, None, :]
        mask = jnp.any(chosen, axis=1)
        top = jnp.max(jnp.where(mask, logits, -jnp.inf), axis=-1, keepdims=True)
        unnorm = jnp.where(mask, jnp.exp(jnp.minimum(logits - top, 0.0)), 0.0)
        gates = unnorm / jnp.sum(unnorm, axis=-1, keepdims=True)
        all_h = lax.all_gather(hidden, group, axis=0, tiled=True)
        all_g = lax.all_gather(gates, group, axis=0, tiled=True)
        all_dy = lax.all_gather(dy_out, group, axis=0, tiled=True)
        my_g = lax.dynamic_slice_in_dim(all_g, lax.axis_index("ep") * local_exp, local_exp, axis=1)
        gate_pre = jnp.einsum("td,mdf->tmf", all_h, w_gate, preferred_element_type=jnp.float32)
        up_pre = jnp.einsum("td,mdf->tmf", all_h, w_up, preferred_element_type=jnp.float32)
        sigma = jax.nn.sigmoid(gate_pre)
        silu = gate_pre * sigma
        act = silu * up_pre
        gated = (act * my_g[:, :, None]).astype(jnp.bfloat16)
        part_out = jnp.einsum("tmf,mfd->td", gated, w_down, preferred_element_type=jnp.float32).astype(jnp.bfloat16)
        y_sum = lax.psum_scatter(part_out, group, scatter_dimension=0, tiled=True)
        y_out = (x_f32 + y_sum.astype(jnp.float32) + out_bias.astype(jnp.float32)).astype(jnp.bfloat16)
        d_act = jnp.einsum("td,mfd->tmf", all_dy, w_down, preferred_element_type=jnp.float32)
        d_gate_part = jnp.sum(act * d_act, axis=-1)
        d_act = d_act * my_g[:, :, None]
        d_gate_pre = (d_act * up_pre * sigma * (1.0 + gate_pre * (1.0 - sigma))).astype(jnp.bfloat16)
        d_up_pre = (d_act * silu).astype(jnp.bfloat16)
        dh_part = (jnp.einsum("tmf,mdf->td", d_gate_pre, w_gate, preferred_element_type=jnp.float32) + jnp.einsum("tmf,mdf->td", d_up_pre, w_up, preferred_element_type=jnp.float32)).astype(jnp.bfloat16)
        dh_expert = lax.psum_scatter(dh_part, group, scatter_dimension=0, tiled=True).astype(jnp.float32)
        d_gate = jnp.einsum("td,tmf->mdf", all_h, d_gate_pre, preferred_element_type=jnp.float32)
        d_up = jnp.einsum("td,tmf->mdf", all_h, d_up_pre, preferred_element_type=jnp.float32)
        d_down = jnp.einsum("tmf,td->mfd", gated, all_dy, preferred_element_type=jnp.float32)
        d_bias = jnp.sum(all_dy.astype(jnp.float32), axis=0)
        d_gates = lax.all_gather(lax.psum(d_gate_part, "tp"), "ep", axis=1, tiled=True)
        d_logits = all_g * (d_gates - jnp.sum(all_g * d_gates, axis=-1, keepdims=True))
        d_router = jnp.einsum("td,te->de", all_h, d_logits.astype(jnp.bfloat16), preferred_element_type=jnp.float32)
        my = lax.axis_index("ep") * lax.axis_size("tp") + lax.axis_index("tp")
        my_dl = lax.dynamic_slice_in_dim(d_logits, my * x_in.shape[0], x_in.shape[0], axis=0)
        dh_total = dh_expert + jnp.einsum("te,de->td", my_dl, w_router, preferred_element_type=jnp.float32)
        d_gain = lax.psum(jnp.sum(dh_total * normed, axis=0), group)
        d_norm = dh_total * gain_f32
        dy_f32 = dy_out.astype(jnp.float32)
        dx_in = (dy_f32 + inv_rms * (d_norm - normed * jnp.mean(d_norm * normed, axis=-1, keepdims=True))).astype(jnp.bfloat16)
        return y_out, dx_in, d_gain, d_router, d_gate, d_up, d_down, d_bias

    return jax.shard_map(device_step, mesh=mesh, in_specs=(tok_spec, P(None), P(None, None), tok_spec, wide_spec, wide_spec, down_spec, P(None), tok_spec), out_specs=(tok_spec, tok_spec, P("dp"), P("dp", None), grad_wide, grad_wide, grad_down, P("dp")), check_vma=False)
```

```python
import functools

import jax
import jax.numpy as jnp
from jax import lax
from jax.experimental import pallas as pl
from jax.experimental.pallas import tpu as pltpu
from jax.sharding import PartitionSpec as P

EPS = 1e-6
CORES = 2
BF16, F32 = jnp.bfloat16, jnp.float32
MESH = pl.DeviceIdType.MESH
NT = (((1,), (1,)), ((), ()))
TN = (((0,), (0,)), ((), ()))


def rows(start, size):
    return pl.ds(pl.multiple_of(start, size & -size), size)


class Place:
    def __init__(self, side):
        ep = lax.axis_index("ep")
        self.side = side
        self.x, self.c, self.y = lax.div(ep, CORES), lax.rem(ep, CORES), lax.axis_index("tp")

    def along(self, axis, step):
        if axis == "x":
            return {"ep": lax.rem(self.x + step + self.side, self.side) * CORES + self.c, "tp": self.y}
        return {"ep": self.x * CORES + self.c, "tp": lax.rem(self.y + step + self.side, self.side)}

    def partner(self):
        return {"ep": self.x * CORES + 1 - self.c, "tp": self.y}


class Half:
    def __init__(self, place, which, blk):
        self.p, self.which, self.blk, n = place, which, blk, place.side
        self.base = which * n
        self.major, self.minor = ("x", "y") if which == 0 else ("y", "x")
        self.m, self.n = (place.x, place.y) if which == 0 else (place.y, place.x)
        self.span = n * blk

    def tile(self, step):
        return self.base + lax.rem(self.m + step + self.p.side, self.p.side)

    def mine(self, part=0, parts=1):
        size = self.span // parts
        return rows(self.p.c * self.span + part * size, size)

    def block(self, step, part=0, parts=1):
        size = self.blk // parts
        return rows(self.p.c * self.span + lax.rem(self.n + step + self.p.side, self.p.side) * self.blk + part * size, size)


class Gather:
    COPIES = 12

    def __init__(self, halves, own, buf, send, recv):
        self.halves, self.own, self.buf, self.send, self.recv = halves, own, buf, send, recv

    def copy(self, h, k, src, dst, target):
        i = h.which * self.COPIES + k
        return pltpu.make_async_remote_copy(src_ref=src, dst_ref=dst, send_sem=self.send.at[i], recv_sem=self.recv.at[i], device_id=target, device_id_type=MESH)

    def make(self, h, k):
        b, p = self.buf, h.p
        same = lambda t, r, target: self.copy(h, k, b.at[t, r], b.at[t, r], target)
        if k < 2:
            return self.copy(h, k, self.own.at[pl.ds(h.which * h.blk, h.blk)], b.at[h.tile(0), h.block(0)], p.along(h.minor, 1 - 2 * k))
        if k < 4:
            s = 1 - 2 * (k - 2)
            return same(h.tile(0), h.block(-s, k - 2, 2), p.along(h.minor, s))
        if k < 6:
            return same(h.tile(0), h.mine(), p.along(h.major, 1 - 2 * (k - 4)))
        if k < 8:
            s = 1 - 2 * (k - 6)
            return same(h.tile(-s), h.mine(k - 6, 2), p.along(h.major, s))
        return same(h.tile((0, -1, 1, 2)[k - 8]), h.mine(), p.partner())

    def own_copy(self, h, sem):
        return pltpu.make_async_copy(self.own.at[pl.ds(h.which * h.blk, h.blk)], self.buf.at[h.tile(0), h.block(0)], sem)

    def start(self, *ks):
        for k in ks:
            for h in self.halves:
                self.make(h, k).start()

    def wait(self, *ks):
        for k in ks:
            for h in self.halves:
                self.make(h, k).wait_recv()

    def finish(self):
        for k in range(self.COPIES):
            for h in self.halves:
                self.make(h, k).wait_send()

    def begin(self, local):
        self.start(0, 1)
        for h in self.halves:
            self.own_copy(h, local.at[h.which]).start()

    def step(self, k, local=None):
        if k == 0:
            for h in self.halves:
                self.own_copy(h, local.at[h.which]).wait()
            self.wait(0, 1)
            self.start(2, 3)
        elif k == 1:
            self.wait(2, 3)
            self.start(4, 5, 8)
        elif k == 2:
            self.wait(4, 5)
            self.start(6, 7, 9, 10)
        elif k == 3:
            self.wait(6, 7)
            self.start(11)
        elif k == 4:
            self.wait(8)
        elif k == 5:
            self.wait(9, 10)
        else:
            self.wait(11)


class Scatter:
    COPIES = 8

    def __init__(self, halves, part, swap, big, small, out, send, recv, swap_send, swap_recv):
        self.halves, self.part, self.swap, self.big, self.small, self.out = halves, part, swap, big, small, out
        self.send, self.recv, self.swap_send, self.swap_recv = send, recv, swap_send, swap_recv

    def swap_copy(self, t, p, span):
        theirs = rows((1 - p.c) * span, span)
        return pltpu.make_async_remote_copy(src_ref=self.part.at[t, theirs], dst_ref=self.swap.at[t], send_sem=self.swap_send.at[t], recv_sem=self.swap_recv.at[t], device_id=p.partner(), device_id_type=MESH)

    def swapped(self, h, step):
        t = h.tile(step)
        self.swap_copy(t, h.p, h.span).wait_recv()
        self.add(t, h.mine(), self.swap[t])

    def add(self, t, r, *terms):
        total = self.part[t, r].astype(F32)
        for term in terms:
            total = total + term.astype(F32)
        self.part[t, r] = total.astype(BF16)

    def land(self, h, k):
        s, b = h.span, h.blk
        if k < 2:
            return self.big.at[h.which, pl.ds(k * (s // 2), s // 2)]
        if k < 4:
            return self.big.at[h.which, pl.ds(s + (k - 2) * s, s)]
        if k < 6:
            return self.small.at[h.which, pl.ds((k - 4) * (b // 2), b // 2)]
        return self.small.at[h.which, pl.ds(b + (k - 6) * b, b)]

    def make(self, h, k):
        s = 1 - 2 * (k % 2)
        if k < 2:
            src, axis = self.part.at[h.tile(2), h.mine(k, 2)], h.major
        elif k < 4:
            src, axis = self.part.at[h.tile(s), h.mine()], h.major
        elif k < 6:
            src, axis = self.part.at[h.tile(0), h.block(2, k - 4, 2)], h.minor
        else:
            src, axis = self.part.at[h.tile(0), h.block(s)], h.minor
        i = h.which * self.COPIES + k
        return pltpu.make_async_remote_copy(src_ref=src, dst_ref=self.land(h, k), send_sem=self.send.at[i], recv_sem=self.recv.at[i], device_id=h.p.along(axis, s), device_id_type=MESH)

    def step(self, k):
        for h in self.halves:
            if k == 0:
                self.swapped(h, 2)
                self.make(h, 0).start()
                self.make(h, 1).start()
            elif k == 1:
                for q in (1, -1, 0):
                    self.swapped(h, q)
            elif k == 2:
                for d in (0, 1):
                    self.make(h, d).wait_recv()
                    self.add(h.tile(1 - 2 * d), h.mine(d, 2), self.land(h, d)[...])
                    self.make(h, 2 + d).start()
            elif k == 3:
                self.make(h, 2).wait_recv()
                self.make(h, 3).wait_recv()
                self.add(h.tile(0), h.mine(), self.land(h, 2)[...], self.land(h, 3)[...])
                self.make(h, 4).start()
                self.make(h, 5).start()
            elif k == 4:
                for d in (0, 1):
                    self.make(h, 4 + d).wait_recv()
                    self.add(h.tile(0), h.block(1 - 2 * d, d, 2), self.land(h, 4 + d)[...])
                    self.make(h, 6 + d).start()
            elif k == 5:
                self.make(h, 6).wait_recv()
                self.make(h, 7).wait_recv()
                total = self.part[h.tile(0), h.block(0)].astype(F32) + self.land(h, 6)[...].astype(F32) + self.land(h, 7)[...].astype(F32)
                self.out[pl.ds(h.which * h.blk, h.blk)] = total
            else:
                for i in range(self.COPIES):
                    self.make(h, i).wait_send()


def moe_kernel(side, d, e_loc, ff, h_in, dy_in, sel, sel_t, wg_hbm, wu_hbm, wd_hbm,
               y_sum, dh_sum, d_bias, d_router_t, d_logits_t, dwg_hbm, dwu_hbm, dwd_hbm,
               hid, dys, dgs, dg_own, w_gu, w_d, gated, d_gu, part_y, part_dh, swap, big_y, big_dh, small_y, small_dh,
               gu_s, gx_s, da_s, wd_s, bias_s,
               w_sem, local, g_send, g_recv, s_send, s_recv, swap_send, swap_recv, out_sem):
    place = Place(side)
    n_tile = 2 * side
    blk = h_in.shape[0] // 2
    halves = [Half(place, 0, blk), Half(place, 1, blk)]
    tile_rows = hid.shape[1]
    span = tile_rows // CORES

    weights = []
    for e in range(e_loc):
        weights.append(pltpu.make_async_copy(wg_hbm.at[e], w_gu.at[:, pl.ds(2 * e * ff, ff)], w_sem.at[3 * e]))
        weights.append(pltpu.make_async_copy(wu_hbm.at[e], w_gu.at[:, pl.ds((2 * e + 1) * ff, ff)], w_sem.at[3 * e + 1]))
        weights.append(pltpu.make_async_copy(wd_hbm.at[e], w_d.at[pl.ds(e * ff, ff)], w_sem.at[3 * e + 2]))

    barrier = pltpu.get_barrier_semaphore()
    peers = [place.along("x", 1), place.along("x", -1), place.along("y", 1), place.along("y", -1), place.partner()]
    for peer in peers:
        pl.semaphore_signal(barrier, inc=1, device_id=peer, device_id_type=MESH)
    for w in weights:
        w.start()
    pl.semaphore_wait(barrier, len(peers))

    gather_h = Gather(halves, h_in, hid, g_send.at[0], g_recv.at[0])
    gather_dy = Gather(halves, dy_in, dys, g_send.at[1], g_recv.at[1])
    gather_dg = Gather(halves, dg_own, dgs, g_send.at[2], g_recv.at[2])
    scat_y = Scatter(halves, part_y, swap.at[0], big_y, small_y, y_sum, s_send.at[0], s_recv.at[0], swap_send.at[0], swap_recv.at[0])
    scat_dh = Scatter(halves, part_dh, swap.at[1], big_dh, small_dh, dh_sum, s_send.at[1], s_recv.at[1], swap_send.at[1], swap_recv.at[1])

    gather_h.begin(local.at[0])
    gather_dy.begin(local.at[1])
    gather_h.step(0, local.at[0])
    gather_dy.step(0, local.at[1])
    for w in weights:
        w.wait()
    gather_h.step(1)
    gather_dy.step(1)

    lane = lax.broadcasted_iota(jnp.int32, (tile_rows, 128), 1)

    def tile_step(i, _):
        @pl.when(i == 0)
        def _():
            gather_h.step(4)
            gather_dy.step(4)

        @pl.when(i == 2)
        def _():
            gather_h.step(2)
            gather_dy.step(2)
            gather_h.step(5)
            gather_dy.step(5)

        @pl.when(i == 6)
        def _():
            gather_h.step(3)
            gather_dy.step(3)
            gather_h.step(6)
            gather_dy.step(6)

        j, which = lax.div(i, 2), lax.rem(i, 2)
        off = j + lax.div(j, 2) - 2 * lax.div(j, 3)
        t = which * side + lax.rem(place.x * (1 - which) + place.y * which + off, side)
        gu_s[...] = jnp.dot(hid[t, :, pl.ds(0, d)], w_gu[...], preferred_element_type=F32)
        gx_s[...] = jnp.dot(hid[t, :, pl.ds(d, 128)], sel[...], preferred_element_type=F32)
        da_s[...] = lax.dot_general(dys[t], w_d[...], NT, preferred_element_type=F32)
        bias_s[t] = jnp.sum(dys[t].astype(F32), axis=0, keepdims=True)
        sums = jnp.zeros((tile_rows, 128), F32)
        for e in range(e_loc):
            pre, up = gu_s[:, pl.ds(2 * e * ff, ff)], gu_s[:, pl.ds((2 * e + 1) * ff, ff)]
            gate, da = gx_s[:, pl.ds(e * ff, ff)], da_s[:, pl.ds(e * ff, ff)]
            sigma = jax.nn.sigmoid(pre)
            silu = pre * sigma
            act = silu * up
            gated[t, :, pl.ds(e * ff, ff)] = (act * gate).astype(BF16)
            sums = sums + jnp.where(lane == e, jnp.sum(act * da, axis=1, keepdims=True), 0.0)
            da = da * gate
            d_gu[t, :, pl.ds(2 * e * ff, ff)] = (da * up * sigma * (1.0 + pre * (1.0 - sigma))).astype(BF16)
            d_gu[t, :, pl.ds((2 * e + 1) * ff, ff)] = (da * silu).astype(BF16)
        dg_own[rows(t * 8, 8)] = jnp.transpose(sums)[:8]
        part_y[t] = jnp.dot(gated[t], w_d[...], preferred_element_type=F32).astype(BF16)
        scat_y.swap_copy(t, place, span).start()
        part_dh[t] = lax.dot_general(d_gu[t], w_gu[...], NT, preferred_element_type=F32).astype(BF16)
        scat_dh.swap_copy(t, place, span).start()
        return 0

    lax.fori_loop(0, n_tile, tile_step, 0)

    gather_dg.begin(local.at[2])
    d_bias[...] = jnp.sum(bias_s[...], axis=0)
    scat_y.step(0)
    gather_dg.step(0, local.at[2])
    scat_dh.step(0)
    gather_dg.step(1)
    scat_y.step(1)
    scat_dh.step(1)

    m_blk = gu_s.shape[0]
    n_m = d // m_blk

    def wide_copies(mb):
        out = []
        for e in range(e_loc):
            for j, ref in enumerate((dwg_hbm, dwu_hbm)):
                out.append(pltpu.make_async_copy(gu_s.at[:, pl.ds((2 * e + j) * ff, ff)], ref.at[e, rows(mb * m_blk, m_blk)], out_sem.at[2 * e + j]))
        return out

    def wide_step(mb, _):
        @pl.when(mb > 0)
        def _():
            for cp in wide_copies(mb - 1):
                cp.wait()
        a = hid[:, :, rows(mb * m_blk, m_blk)].reshape(n_tile * tile_rows, m_blk)
        b = d_gu[...].reshape(n_tile * tile_rows, 2 * e_loc * ff)
        gu_s[...] = lax.dot_general(a, b, TN, preferred_element_type=F32)
        for cp in wide_copies(mb):
            cp.start()

        @pl.when(mb == 1)
        def _():
            scat_y.step(2)
            gather_dg.step(2)

        @pl.when(mb == 2)
        def _():
            scat_dh.step(2)
            gather_dg.step(3)
        return 0

    lax.fori_loop(0, n_m, wide_step, 0)
    for cp in wide_copies(n_m - 1):
        cp.wait()

    n_blk = wd_s.shape[1]

    def down_copies(nb):
        return [pltpu.make_async_copy(wd_s.at[pl.ds(e * ff, ff)], dwd_hbm.at[e, :, rows(nb * n_blk, n_blk)], out_sem.at[e]) for e in range(e_loc)]

    def down_step(nb, _):
        @pl.when(nb > 0)
        def _():
            for cp in down_copies(nb - 1):
                cp.wait()
        a = gated[...].reshape(n_tile * tile_rows, e_loc * ff)
        b = dys[:, :, rows(nb * n_blk, n_blk)].reshape(n_tile * tile_rows, n_blk)
        wd_s[...] = lax.dot_general(a, b, TN, preferred_element_type=F32)
        for cp in down_copies(nb):
            cp.start()
        return 0

    lax.fori_loop(0, d // n_blk, down_step, 0)
    for cp in down_copies(d // n_blk - 1):
        cp.wait()

    scat_y.step(3)
    gather_dg.step(4)
    gather_dg.step(5)
    gather_dg.step(6)
    d_router_t[...] = jnp.zeros_like(d_router_t)
    for t in range(n_tile):
        which, tl = t // side, t % side
        pieces = []
        for ep in range(side * CORES):
            px, pc = ep // CORES, ep % CORES
            total = None
            for py in range(side):
                if which == 0:
                    term = dgs[px, pl.ds((pc * side + py) * blk + tl * 8, 8)]
                else:
                    term = dgs[side + py, pl.ds((pc * side + px) * blk + tl * 8, 8)]
                total = term if total is None else total + term
            pieces.append(total)
        d_g = jnp.concatenate(pieces, axis=0)
        g_t = lax.dot_general(sel_t[...], hid[t, :, pl.ds(d, 128)], NT, preferred_element_type=F32)
        d_l = g_t * (d_g - jnp.sum(g_t * d_g, axis=0, keepdims=True))
        d_logits_t[t] = d_l
        d_router_t[...] += jnp.dot(d_l.astype(BF16), hid[t, :, pl.ds(0, d)], preferred_element_type=F32)

    scat_y.step(4)
    scat_dh.step(3)
    scat_y.step(5)
    scat_dh.step(4)
    scat_dh.step(5)
    for g in (gather_h, gather_dy, gather_dg):
        g.finish()
    for s in (scat_y, scat_dh):
        s.step(6)
        for t in range(n_tile):
            s.swap_copy(t, place, span).wait_send()


def moe(mesh, h_ext, dy, sel, sel_t, w_gate, w_up, w_down):
    side = mesh.shape["tp"]
    n_tok, d = dy.shape
    e_loc, _, ff = w_gate.shape
    tile_rows = CORES * side * n_tok // 2
    span = tile_rows // CORES
    n_tile = 2 * side
    n_ep = side * CORES
    dx = h_ext.shape[1]
    vm = pl.BlockSpec(memory_space=pltpu.VMEM)
    hbm = pl.BlockSpec(memory_space=pl.ANY)
    blk = n_tok // 2
    n_g, n_s = 2 * Gather.COPIES, 2 * Scatter.COPIES
    return pl.pallas_call(
        functools.partial(moe_kernel, side, d, e_loc, ff),
        out_shape=(
            jax.ShapeDtypeStruct((n_tok, d), F32),
            jax.ShapeDtypeStruct((n_tok, d), F32),
            jax.ShapeDtypeStruct((1, d), F32),
            jax.ShapeDtypeStruct((n_ep * 8, d), F32),
            jax.ShapeDtypeStruct((n_tile, n_ep * 8, tile_rows), F32),
            jax.ShapeDtypeStruct(w_gate.shape, F32),
            jax.ShapeDtypeStruct(w_up.shape, F32),
            jax.ShapeDtypeStruct(w_down.shape, F32),
        ),
        in_specs=[vm, vm, vm, vm, hbm, hbm, hbm],
        out_specs=(vm, vm, vm, vm, vm, hbm, hbm, hbm),
        scratch_shapes=[
            pltpu.VMEM((n_tile, tile_rows, dx), BF16),
            pltpu.VMEM((n_tile, tile_rows, d), BF16),
            pltpu.VMEM((n_tile, tile_rows, tile_rows), F32),
            pltpu.VMEM((n_tok, tile_rows), F32),
            pltpu.VMEM((d, 2 * e_loc * ff), BF16),
            pltpu.VMEM((e_loc * ff, d), BF16),
            pltpu.VMEM((n_tile, tile_rows, e_loc * ff), BF16),
            pltpu.VMEM((n_tile, tile_rows, 2 * e_loc * ff), BF16),
            pltpu.VMEM((n_tile, tile_rows, d), BF16),
            pltpu.VMEM((n_tile, tile_rows, d), BF16),
            pltpu.VMEM((2, n_tile, span, d), BF16),
            pltpu.VMEM((2, 3 * span, d), BF16),
            pltpu.VMEM((2, 3 * span, d), BF16),
            pltpu.VMEM((2, 3 * blk, d), BF16),
            pltpu.VMEM((2, 3 * blk, d), BF16),
            pltpu.VMEM((tile_rows, 2 * e_loc * ff), F32),
            pltpu.VMEM((tile_rows, e_loc * ff), F32),
            pltpu.VMEM((tile_rows, e_loc * ff), F32),
            pltpu.VMEM((e_loc * ff, 256), F32),
            pltpu.VMEM((n_tile, 1, d), F32),
            pltpu.SemaphoreType.DMA((3 * e_loc,)),
            pltpu.SemaphoreType.DMA((3, 2)),
            pltpu.SemaphoreType.DMA((3, n_g)),
            pltpu.SemaphoreType.DMA((3, n_g)),
            pltpu.SemaphoreType.DMA((2, n_s)),
            pltpu.SemaphoreType.DMA((2, n_s)),
            pltpu.SemaphoreType.DMA((2, n_tile)),
            pltpu.SemaphoreType.DMA((2, n_tile)),
            pltpu.SemaphoreType.DMA((2 * e_loc,)),
        ],
        compiler_params=pltpu.CompilerParams(collective_id=0, has_side_effects=True, vmem_limit_bytes=67043328),
        name="moe",
    )(h_ext, dy, sel, sel_t, w_gate, w_up, w_down)


def solution(mesh):
    tok_spec = P(("dp", "ep", "tp"), None)
    wide_spec = P("ep", None, "tp")
    down_spec = P("ep", "tp", None)
    grad_wide = P(("dp", "ep"), None, "tp")
    grad_down = P(("dp", "ep"), "tp", None)
    group = ("ep", "tp")
    side = mesh.shape["tp"]
    assert mesh.shape["ep"] == side * CORES

    def device_step(x_in, norm_gain, w_router, expert_idx, w_gate, w_up, w_down, out_bias, dy_out):
        n_tok, d_model = x_in.shape
        n_exp = w_router.shape[1]
        local_exp, _, ff = w_gate.shape
        n_ep = n_exp // local_exp
        blk = n_tok // 2
        x_f32 = x_in.astype(F32)
        inv_rms = lax.rsqrt(jnp.mean(x_f32 * x_f32, axis=-1, keepdims=True) + EPS)
        normed = x_f32 * inv_rms
        gain_f32 = norm_gain.astype(F32)
        hidden = (normed * gain_f32).astype(BF16)
        logits = jnp.dot(hidden, w_router, preferred_element_type=F32)
        chosen = expert_idx[:, :, None] == jnp.arange(n_exp)[None, None, :]
        mask = jnp.any(chosen, axis=1)
        top = jnp.max(jnp.where(mask, logits, -jnp.inf), axis=-1, keepdims=True)
        unnorm = jnp.where(mask, jnp.exp(jnp.minimum(logits - top, 0.0)), 0.0)
        gates = unnorm / jnp.sum(unnorm, axis=-1, keepdims=True)
        hi = lax.reduce_precision(gates, 8, 7)
        mid = lax.reduce_precision(gates - hi, 8, 7)
        lo = gates - hi - mid
        zeros = jnp.zeros((n_tok, 128 - 3 * n_exp), F32)
        h_ext = jnp.concatenate([hidden, jnp.concatenate([hi, mid, lo, zeros], axis=1).astype(BF16)], axis=1)
        ep, tp = lax.axis_index("ep"), lax.axis_index("tp")
        lane = jnp.arange(128)
        lane_e = jnp.where(lane < 3 * n_exp, lane % n_exp, n_exp)
        sel = (lane_e[:, None] == (ep * local_exp + jnp.arange(local_exp * ff) // ff)[None, :]).astype(BF16)
        slot = jnp.arange(n_ep * 8)
        slot_e = jnp.where(slot % 8 < local_exp, slot // 8 * local_exp + slot % 8, n_exp + 1)
        sel_t = (slot_e[:, None] == lane_e[None, :]).astype(BF16)
        y_sum, dh_sum, d_bias, dr_t, dl_t, d_gate, d_up, d_down = moe(mesh, h_ext, dy_out, sel, sel_t, w_gate, w_up, w_down)
        y_out = (x_f32 + y_sum + out_bias.astype(F32)).astype(BF16)
        d_router = dr_t.reshape(n_ep, 8, d_model)[:, :local_exp].reshape(n_exp, d_model).T
        x, c = ep // CORES, ep % CORES
        own_a = lax.dynamic_slice(dl_t, (x, 0, (c * side + tp) * blk), (1, n_ep * 8, blk))[0]
        own_b = lax.dynamic_slice(dl_t, (side + tp, 0, (c * side + x) * blk), (1, n_ep * 8, blk))[0]
        own_dl = jnp.concatenate([own_a, own_b], axis=1).reshape(n_ep, 8, n_tok)[:, :local_exp].reshape(n_exp, n_tok)
        dh_total = dh_sum + jnp.einsum("et,de->td", own_dl.astype(BF16), w_router, preferred_element_type=F32)
        d_gain = lax.psum(jnp.sum(dh_total * normed, axis=0), group)
        d_norm = dh_total * gain_f32
        dx_in = (dy_out.astype(F32) + inv_rms * (d_norm - normed * jnp.mean(d_norm * normed, axis=-1, keepdims=True))).astype(BF16)
        return y_out, dx_in, d_gain, d_router, d_gate, d_up, d_down, d_bias.reshape(d_model)

    return jax.shard_map(device_step, mesh=mesh, in_specs=(tok_spec, P(None), P(None, None), tok_spec, wide_spec, wide_spec, down_spec, P(None), tok_spec), out_specs=(tok_spec, tok_spec, P("dp"), P("dp", None), grad_wide, grad_wide, grad_down, P("dp")), check_vma=False)
```

```python
import functools

import jax
import jax.numpy as jnp
from jax import lax
from jax.experimental import pallas as pl
from jax.experimental.pallas import tpu as pltpu
from jax.sharding import PartitionSpec as P

EPS = 1e-6
CORES = 2
BF16, F32 = jnp.bfloat16, jnp.float32
MESH = pl.DeviceIdType.MESH
NT = (((1,), (1,)), ((), ()))
TN = (((0,), (0,)), ((), ()))


def rows(start, size):
    return pl.ds(pl.multiple_of(start, size & -size), size)


class Place:
    def __init__(self, side):
        ep = lax.axis_index("ep")
        self.side = side
        self.x, self.c, self.y = lax.div(ep, CORES), lax.rem(ep, CORES), lax.axis_index("tp")

    def along(self, axis, step):
        if axis == "x":
            return {"ep": lax.rem(self.x + step + self.side, self.side) * CORES + self.c, "tp": self.y}
        return {"ep": self.x * CORES + self.c, "tp": lax.rem(self.y + step + self.side, self.side)}

    def partner(self):
        return {"ep": self.x * CORES + 1 - self.c, "tp": self.y}


class Half:
    def __init__(self, place, which, blk):
        self.p, self.which, self.blk, n = place, which, blk, place.side
        self.base = which * n
        self.major, self.minor = ("x", "y") if which == 0 else ("y", "x")
        self.m, self.n = (place.x, place.y) if which == 0 else (place.y, place.x)
        self.span = n * blk

    def tile(self, step):
        return self.base + lax.rem(self.m + step + self.p.side, self.p.side)

    def mine(self, part=0, parts=1):
        size = self.span // parts
        return rows(self.p.c * self.span + part * size, size)

    def block(self, step, part=0, parts=1):
        size = self.blk // parts
        return rows(self.p.c * self.span + lax.rem(self.n + step + self.p.side, self.p.side) * self.blk + part * size, size)


class Gather:
    COPIES = 17

    def __init__(self, halves, own, buf, send, recv):
        self.halves, self.own, self.buf, self.send, self.recv = halves, own, buf, send, recv

    def copy(self, h, k, src, dst, target):
        i = h.which * self.COPIES + k
        return pltpu.make_async_remote_copy(src_ref=src, dst_ref=dst, send_sem=self.send.at[i], recv_sem=self.recv.at[i], device_id=target, device_id_type=MESH)

    def make(self, h, k):
        b, p = self.buf, h.p
        same = lambda t, r, target: self.copy(h, k, b.at[t, r], b.at[t, r], target)
        s, d = 1 - 2 * (k % 2), k % 2
        if k < 2:
            return self.copy(h, k, self.own.at[pl.ds(h.which * h.blk, h.blk)], b.at[h.tile(0), h.block(0)], p.along(h.minor, s))
        if k < 4:
            return same(h.tile(0), h.block(-s, d, 2), p.along(h.minor, s))
        if k < 6:
            return same(h.tile(0), h.mine(d, 2), p.along(h.major, s))
        if k < 8:
            return same(h.tile(0), h.mine(1 - d, 2), p.along(h.major, s))
        if k < 10:
            return same(h.tile(-s), h.mine(d, 2), p.along(h.major, s))
        if k == 10:
            return same(h.tile(0), h.mine(), p.partner())
        step, part = ((-1, 0), (1, 1), (-1, 1), (1, 0), (2, 0), (2, 1))[k - 11]
        return same(h.tile(step), h.mine(part, 2), p.partner())

    def own_copy(self, h, sem):
        return pltpu.make_async_copy(self.own.at[pl.ds(h.which * h.blk, h.blk)], self.buf.at[h.tile(0), h.block(0)], sem)

    def start(self, *ks):
        for k in ks:
            for h in self.halves:
                self.make(h, k).start()

    def wait(self, *ks):
        for k in ks:
            for h in self.halves:
                self.make(h, k).wait_recv()

    def finish(self):
        for k in range(self.COPIES):
            for h in self.halves:
                self.make(h, k).wait_send()

    def begin(self, local):
        self.start(0, 1)
        for h in self.halves:
            self.own_copy(h, local.at[h.which]).start()

    def relay_minor(self, local):
        for h in self.halves:
            self.own_copy(h, local.at[h.which]).wait()
        self.wait(0, 1)
        self.start(2, 3)

    def share_own(self):
        self.wait(2, 3)
        self.start(10)

    def send_major(self):
        self.start(4, 5, 6, 7)

    def relay_major(self):
        self.wait(4, 5)
        self.start(8, 9, 11, 12)

    def share_near(self):
        self.wait(6, 7)
        self.start(13, 14)

    def share_far(self):
        self.wait(8, 9)
        self.start(15, 16)


class Scatter:
    COPIES = 12

    def __init__(self, halves, part, big, small, send, recv):
        self.halves, self.part, self.big, self.small, self.send, self.recv = halves, part, big, small, send, recv

    def piece(self, h, part, parts=2):
        size = h.span // parts
        return pl.ds(part * size, size)

    def block(self, h, step, part=0, parts=1):
        size = h.blk // parts
        return rows(lax.rem(h.n + step + h.p.side, h.p.side) * h.blk + part * size, size)

    def add(self, t, r, *terms):
        total = self.part[t, r].astype(F32)
        for term in terms:
            total = total + term.astype(F32)
        self.part[t, r] = total.astype(BF16)

    def land(self, h, k):
        if k < 6:
            return self.big.at[h.which, pl.ds(k * (h.span // 2), h.span // 2)]
        return self.small.at[h.which, pl.ds((k - 6) * (h.blk // 2), h.blk // 2)]

    def make(self, h, k):
        s, d = 1 - 2 * (k % 2), k % 2
        if k < 2:
            src = self.part.at[h.tile(2), self.piece(h, d)]
        elif k < 4:
            src = self.part.at[h.tile(s), self.piece(h, 1 - d)]
        elif k < 6:
            src = self.part.at[h.tile(s), self.piece(h, d)]
        elif k < 8:
            src = self.part.at[h.tile(0), self.block(h, 2, d, 2)]
        elif k < 10:
            src = self.part.at[h.tile(0), self.block(h, s, 1 - d, 2)]
        else:
            src = self.part.at[h.tile(0), self.block(h, s, d, 2)]
        i = h.which * self.COPIES + k
        axis = h.major if k < 6 else h.minor
        return pltpu.make_async_remote_copy(src_ref=src, dst_ref=self.land(h, k), send_sem=self.send.at[i], recv_sem=self.recv.at[i], device_id=h.p.along(axis, s), device_id_type=MESH)

    def start(self, h, *ks):
        for k in ks:
            self.make(h, k).start()

    def got(self, h, k):
        self.make(h, k).wait_recv()
        return self.land(h, k)[...]

    def begin(self):
        for h in self.halves:
            self.start(h, 0, 1)
        for h in self.halves:
            self.start(h, 2, 3)

    def relay_major(self):
        for h in self.halves:
            for d in (0, 1):
                self.add(h.tile(1 - 2 * d), self.piece(h, d), self.got(h, d))
                self.start(h, 4 + d)

    def turn(self):
        for h in self.halves:
            self.add(h.tile(0), self.piece(h, 0), self.got(h, 3), self.got(h, 4))
            self.add(h.tile(0), self.piece(h, 1), self.got(h, 2), self.got(h, 5))
            self.start(h, 6, 7, 8, 9)

    def relay_minor(self):
        for h in self.halves:
            for d in (0, 1):
                self.add(h.tile(0), self.block(h, 1 - 2 * d, d, 2), self.got(h, 6 + d))
                self.start(h, 10 + d)

    def total(self, h):
        mine = self.part[h.tile(0), self.block(h, 0)].astype(F32)
        low = self.got(h, 9).astype(F32) + self.got(h, 10).astype(F32)
        high = self.got(h, 8).astype(F32) + self.got(h, 11).astype(F32)
        return mine + jnp.concatenate([low, high], axis=0)

    def finish(self):
        for h in self.halves:
            for k in range(self.COPIES):
                self.make(h, k).wait_send()


def moe_kernel(side, d, e_loc, ff, n_exp, h_in, dy_in, x_ref, gain_ref, bias_ref, sel, sel_t, w_rt, pick, wg_hbm, wu_hbm, wd_hbm,
               y_ref, dx_ref, d_gain, d_bias, d_router_t, dwg_hbm, dwu_hbm, dwd_hbm,
               hid, dys, dgs, dg_own, w_gu, w_d, gated, d_gu, part_y, part_dh, stage, swap, big_y, big_dh, small_y, small_dh,
               gu, gx_s, da_s, wd_s, bias_s, dl_s, dr_s, ar1, ar2,
               w_sem, local, g_send, g_recv, s_send, s_recv, stage_send, swap_recv, credit, out_sem, ar_send, ar_recv):
    place = Place(side)
    n_tile = 2 * side
    n_ep = side * CORES
    blk = h_in.shape[0] // 2
    halves = [Half(place, 0, blk), Half(place, 1, blk)]
    tile_rows = hid.shape[1]
    span = tile_rows // CORES
    mine, theirs = rows(place.c * span, span), rows((1 - place.c) * span, span)
    me_ep = lax.axis_index("ep")

    weights = []
    for e in range(e_loc):
        weights.append(pltpu.make_async_copy(wg_hbm.at[e], w_gu.at[:, pl.ds(2 * e * ff, ff)], w_sem.at[3 * e]))
        weights.append(pltpu.make_async_copy(wu_hbm.at[e], w_gu.at[:, pl.ds((2 * e + 1) * ff, ff)], w_sem.at[3 * e + 1]))
        weights.append(pltpu.make_async_copy(wd_hbm.at[e], w_d.at[pl.ds(e * ff, ff)], w_sem.at[3 * e + 2]))

    ep_peers = [{"ep": lax.rem(me_ep + o, n_ep), "tp": place.y} for o in range(1, n_ep)]
    tp_peers = [{"ep": me_ep, "tp": lax.rem(place.y + o, side)} for o in range(1, side)]
    barrier = pltpu.get_barrier_semaphore()
    for peer in ep_peers + tp_peers:
        pl.semaphore_signal(barrier, inc=1, device_id=peer, device_id_type=MESH)
    for w in weights:
        w.start()
    pl.semaphore_wait(barrier, n_ep + side - 2)

    gather_h = Gather(halves, h_in, hid, g_send.at[0], g_recv.at[0])
    gather_dy = Gather(halves, dy_in, dys, g_send.at[1], g_recv.at[1])
    gather_dg = Gather(halves, dg_own, dgs, g_send.at[2], g_recv.at[2])
    scat_y = Scatter(halves, part_y, big_y, small_y, s_send.at[0], s_recv.at[0])
    scat_dh = Scatter(halves, part_dh, big_dh, small_dh, s_send.at[1], s_recv.at[1])

    gather_h.begin(local.at[0])
    gather_dy.begin(local.at[1])
    gather_h.relay_minor(local.at[0])
    gather_dy.relay_minor(local.at[1])
    gather_h.share_own()
    gather_h.send_major()
    gather_dy.share_own()
    for w in weights:
        w.wait()

    lane = lax.broadcasted_iota(jnp.int32, (tile_rows, 128), 1)

    def index_of(s):
        i = s - 2 * jnp.minimum(1, lax.div(s, 2)) - 6 * jnp.minimum(1, lax.div(s, 10))
        j, which = lax.div(i, 2), lax.rem(i, 2)
        off = j + lax.div(j, 2) - 2 * lax.div(j, 3)
        return which * side + lax.rem(place.x * (1 - which) + place.y * which + off, side)

    def is_back(s):
        return jnp.logical_or(jnp.logical_and(s >= 2, s < 4), s >= 10)

    def swap_copy(s, kind, t):
        slot = lax.rem(s, 2)
        return pltpu.make_async_remote_copy(src_ref=stage.at[slot, theirs], dst_ref=swap.at[t], send_sem=stage_send.at[slot], recv_sem=swap_recv.at[kind, t], device_id=place.partner(), device_id_type=MESH)

    def settle(s):
        t = index_of(s)

        def take(kind, part):
            swap_copy(s, kind, t).wait_recv()
            part[t] = (part[t].astype(F32) + swap[t].astype(F32)).astype(BF16)

        @pl.when(jnp.logical_not(is_back(s)))
        def _():
            take(0, part_y)
            pl.semaphore_signal(credit, inc=1, device_id=place.partner(), device_id_type=MESH)

        @pl.when(is_back(s))
        def _():
            take(1, part_dh)

    def hand_over(s, kind, t, part, value):
        @pl.when(s >= 1)
        def _():
            settle(s - 1)

        @pl.when(s >= 2)
        def _():
            swap_copy(s, kind, t).wait_send()

        slot = lax.rem(s, 2)
        stage[slot] = value().astype(BF16)
        part[t] = stage[slot, mine]
        if kind == 1:
            pl.semaphore_wait(credit, 1)
        swap_copy(s, kind, t).start()

    def tile_step(s, _):
        t = index_of(s)

        def at(k, *actions):
            @pl.when(s == k)
            def _():
                for action in actions:
                    action()

        at(0, lambda: gather_h.wait(10))
        at(2, gather_h.relay_major, gather_dy.send_major, lambda: gather_dy.wait(10))
        at(4, gather_h.share_near, lambda: gather_h.wait(11, 12, 13, 14))
        at(6, gather_h.share_far)
        at(7, gather_dy.relay_major)
        at(8, lambda: gather_h.wait(15, 16))
        at(10, gather_dy.share_near, lambda: gather_dy.wait(11, 12, 13, 14))
        at(11, scat_y.begin)
        at(12, gather_dy.share_far)
        at(14, lambda: gather_dy.wait(15, 16), scat_y.relay_major)

        @pl.when(jnp.logical_not(is_back(s)))
        def _():
            gu[t] = jnp.dot(hid[t, :, pl.ds(0, d)], w_gu[...], preferred_element_type=F32)
            gx_s[...] = jnp.dot(hid[t, :, pl.ds(d, 128)], sel[...], preferred_element_type=F32)
            for e in range(e_loc):
                pre, up = gu[t, :, pl.ds(2 * e * ff, ff)], gu[t, :, pl.ds((2 * e + 1) * ff, ff)]
                act = pre * jax.nn.sigmoid(pre) * up
                gated[t, :, pl.ds(e * ff, ff)] = (act * gx_s[:, pl.ds(e * ff, ff)]).astype(BF16)
            hand_over(s, 0, t, part_y, lambda: jnp.dot(gated[t], w_d[...], preferred_element_type=F32))

        @pl.when(is_back(s))
        def _():
            gx_s[...] = jnp.dot(hid[t, :, pl.ds(d, 128)], sel[...], preferred_element_type=F32)
            da_s[...] = lax.dot_general(dys[t], w_d[...], NT, preferred_element_type=F32)
            bias_s[t] = jnp.sum(dys[t].astype(F32), axis=0, keepdims=True)
            sums = jnp.zeros((tile_rows, 128), F32)
            for e in range(e_loc):
                pre, up = gu[t, :, pl.ds(2 * e * ff, ff)], gu[t, :, pl.ds((2 * e + 1) * ff, ff)]
                gate, da = gx_s[:, pl.ds(e * ff, ff)], da_s[:, pl.ds(e * ff, ff)]
                sigma = jax.nn.sigmoid(pre)
                silu = pre * sigma
                sums = sums + jnp.where(lane == e, jnp.sum(silu * up * da, axis=1, keepdims=True), 0.0)
                da = da * gate
                d_gu[t, :, pl.ds(2 * e * ff, ff)] = (da * up * sigma * (1.0 + pre * (1.0 - sigma))).astype(BF16)
                d_gu[t, :, pl.ds((2 * e + 1) * ff, ff)] = (da * silu).astype(BF16)
            dg_own[rows(t * 8, 8)] = jnp.transpose(sums)[:8]
            hand_over(s, 1, t, part_dh, lambda: lax.dot_general(d_gu[t], w_gu[...], NT, preferred_element_type=F32))

        return 0

    steps = 2 * n_tile
    lax.fori_loop(0, steps, tile_step, 0)

    gather_dg.begin(local.at[2])
    settle(steps - 1)
    scat_dh.begin()
    d_bias[...] = jnp.sum(bias_s[...], axis=0)

    m_blk = tile_rows
    n_m = d // m_blk

    def wide_copies(mb):
        out = []
        for e in range(e_loc):
            for j, ref in enumerate((dwg_hbm, dwu_hbm)):
                out.append(pltpu.make_async_copy(gu.at[mb, :, pl.ds((2 * e + j) * ff, ff)], ref.at[e, rows(mb * m_blk, m_blk)], out_sem.at[mb, 2 * e + j]))
        return out

    def wide_step(mb, _):
        a = hid[:, :, rows(mb * m_blk, m_blk)].reshape(n_tile * tile_rows, m_blk)
        b = d_gu[...].reshape(n_tile * tile_rows, 2 * e_loc * ff)
        gu[mb] = lax.dot_general(a, b, TN, preferred_element_type=F32)
        for cp in wide_copies(mb):
            cp.start()

        def after(k, *actions):
            @pl.when(mb == k)
            def _():
                for action in actions:
                    action()

        after(0, lambda: gather_dg.relay_minor(local.at[2]), scat_y.turn)
        after(1, gather_dg.share_own, gather_dg.send_major)
        after(2, scat_y.relay_minor, scat_dh.relay_major)
        after(4, gather_dg.relay_major)
        after(5, gather_dg.share_near)
        return 0

    lax.fori_loop(0, n_m, wide_step, 0)

    for h in halves:
        r = pl.ds(h.which * blk, blk)
        y_ref[r] = (x_ref[r].astype(F32) + scat_y.total(h) + bias_ref[...].astype(F32)).astype(BF16)

    n_blk = wd_s.shape[2]
    n_n = d // n_blk

    def down_copies(nb):
        slot = lax.rem(nb, 2)
        return [pltpu.make_async_copy(wd_s.at[slot, pl.ds(e * ff, ff)], dwd_hbm.at[e, :, rows(nb * n_blk, n_blk)], out_sem.at[n_m + slot, e]) for e in range(e_loc)]

    def down_step(nb, _):
        @pl.when(nb > 1)
        def _():
            for cp in down_copies(nb - 2):
                cp.wait()
        a = gated[...].reshape(n_tile * tile_rows, e_loc * ff)
        b = dys[:, :, rows(nb * n_blk, n_blk)].reshape(n_tile * tile_rows, n_blk)
        wd_s[lax.rem(nb, 2)] = lax.dot_general(a, b, TN, preferred_element_type=F32)
        for cp in down_copies(nb):
            cp.start()

        @pl.when(nb == 0)
        def _():
            gather_dg.share_far()

        @pl.when(nb == 2)
        def _():
            scat_dh.turn()

        @pl.when(nb == 4)
        def _():
            scat_dh.relay_minor()
        return 0

    lax.fori_loop(0, n_n, down_step, 0)

    gather_dg.wait(10, 11, 12, 13, 14, 15, 16)
    dr_s[...] = jnp.zeros_like(dr_s)
    for t in range(n_tile):
        which, tl = t // side, t % side
        pieces = []
        for ep in range(n_ep):
            px, pc = ep // CORES, ep % CORES
            total = None
            for py in range(side):
                if which == 0:
                    term = dgs[px, pl.ds((pc * side + py) * blk + tl * 8, 8)]
                else:
                    term = dgs[side + py, pl.ds((pc * side + px) * blk + tl * 8, 8)]
                total = term if total is None else total + term
            pieces.append(total)
        d_g = jnp.concatenate(pieces, axis=0)
        g_t = lax.dot_general(sel_t[...], hid[t, :, pl.ds(d, 128)], NT, preferred_element_type=F32)
        d_l = (g_t * (d_g - jnp.sum(g_t * d_g, axis=0, keepdims=True))).astype(BF16)
        dl_s[t] = d_l
        dr_s[...] += jnp.dot(d_l, hid[t, :, pl.ds(0, d)], preferred_element_type=F32)
    d_router_t[...] = jnp.dot(pick[...], dr_s[...], preferred_element_type=F32, precision=lax.Precision.HIGHEST)

    gain = gain_ref[...].astype(F32)
    gain_part = jnp.zeros((1, d), F32)
    for h in halves:
        r = pl.ds(h.which * blk, blk)
        routed = lax.dot_general(dl_s[h.tile(0), :, mine], w_rt[...], TN, preferred_element_type=F32)
        own = jnp.zeros((blk, d), F32)
        for q in range(side):
            own = own + jnp.where(h.n == q, routed[q * blk:(q + 1) * blk], 0.0)
        x_f32 = x_ref[r].astype(F32)
        inv_rms = lax.rsqrt(jnp.mean(x_f32 * x_f32, axis=1, keepdims=True) + EPS)
        normed = x_f32 * inv_rms
        dh = scat_dh.total(h) + own
        gain_part = gain_part + jnp.sum(dh * normed, axis=0, keepdims=True)
        d_norm = dh * gain
        dx_ref[r] = (dy_in[r].astype(F32) + inv_rms * (d_norm - normed * jnp.mean(d_norm * normed, axis=1, keepdims=True))).astype(BF16)

    def spread(buf, slot, peers, first):
        out = []
        for o, peer in enumerate(peers):
            out.append(pltpu.make_async_remote_copy(src_ref=buf.at[slot], dst_ref=buf.at[slot], send_sem=ar_send.at[first + o], recv_sem=ar_recv.at[first + o], device_id=peer, device_id_type=MESH))
        for cp in out:
            cp.start()
        for cp in out:
            cp.wait_recv()
        return out

    ar1[me_ep] = gain_part
    sent = spread(ar1, me_ep, ep_peers, 0)
    ar2[place.y] = jnp.sum(ar1[...], axis=0)
    sent += spread(ar2, place.y, tp_peers, n_ep - 1)
    d_gain[...] = jnp.sum(ar2[...], axis=0)

    for cp in sent:
        cp.wait_send()
    for g in (gather_h, gather_dy, gather_dg):
        g.finish()
    for sc in (scat_y, scat_dh):
        sc.finish()
    for s in (steps - 2, steps - 1):
        swap_copy(s, 1, index_of(s)).wait_send()
    for mb in range(n_m):
        for cp in wide_copies(mb):
            cp.wait()
    for nb in (n_n - 2, n_n - 1):
        for cp in down_copies(nb):
            cp.wait()


def moe(mesh, h_ext, dy, x_in, gain, bias, sel, sel_t, w_rt, pick, w_gate, w_up, w_down):
    side = mesh.shape["tp"]
    n_tok, d = dy.shape
    e_loc, _, ff = w_gate.shape
    tile_rows = CORES * side * n_tok // 2
    span = tile_rows // CORES
    n_tile = 2 * side
    n_ep = side * CORES
    n_exp = n_ep * e_loc
    dx = h_ext.shape[1]
    vm = pl.BlockSpec(memory_space=pltpu.VMEM)
    hbm = pl.BlockSpec(memory_space=pl.ANY)
    blk = n_tok // 2
    n_g, n_s = 2 * Gather.COPIES, 2 * Scatter.COPIES
    n_peer = n_ep + side - 2
    return pl.pallas_call(
        functools.partial(moe_kernel, side, d, e_loc, ff, n_exp),
        out_shape=(
            jax.ShapeDtypeStruct((n_tok, d), BF16),
            jax.ShapeDtypeStruct((n_tok, d), BF16),
            jax.ShapeDtypeStruct((1, d), F32),
            jax.ShapeDtypeStruct((1, d), F32),
            jax.ShapeDtypeStruct((n_exp, d), F32),
            jax.ShapeDtypeStruct(w_gate.shape, F32),
            jax.ShapeDtypeStruct(w_up.shape, F32),
            jax.ShapeDtypeStruct(w_down.shape, F32),
        ),
        in_specs=[vm] * 9 + [hbm] * 3,
        out_specs=(vm, vm, vm, vm, vm, hbm, hbm, hbm),
        scratch_shapes=[
            pltpu.VMEM((n_tile, tile_rows, dx), BF16),
            pltpu.VMEM((n_tile, tile_rows, d), BF16),
            pltpu.VMEM((n_tile, tile_rows, tile_rows), F32),
            pltpu.VMEM((n_tok, tile_rows), F32),
            pltpu.VMEM((d, 2 * e_loc * ff), BF16),
            pltpu.VMEM((e_loc * ff, d), BF16),
            pltpu.VMEM((n_tile, tile_rows, e_loc * ff), BF16),
            pltpu.VMEM((n_tile, tile_rows, 2 * e_loc * ff), BF16),
            pltpu.VMEM((n_tile, span, d), BF16),
            pltpu.VMEM((n_tile, span, d), BF16),
            pltpu.VMEM((2, tile_rows, d), BF16),
            pltpu.VMEM((n_tile, span, d), BF16),
            pltpu.VMEM((2, 3 * span, d), BF16),
            pltpu.VMEM((2, 3 * span, d), BF16),
            pltpu.VMEM((2, 3 * blk, d), BF16),
            pltpu.VMEM((2, 3 * blk, d), BF16),
            pltpu.VMEM((n_tile, tile_rows, 2 * e_loc * ff), F32),
            pltpu.VMEM((tile_rows, e_loc * ff), F32),
            pltpu.VMEM((tile_rows, e_loc * ff), F32),
            pltpu.VMEM((2, e_loc * ff, 256), F32),
            pltpu.VMEM((n_tile, 1, d), F32),
            pltpu.VMEM((n_tile, n_ep * 8, tile_rows), BF16),
            pltpu.VMEM((n_ep * 8, d), F32),
            pltpu.VMEM((n_ep, 1, d), F32),
            pltpu.VMEM((side, 1, d), F32),
            pltpu.SemaphoreType.DMA((3 * e_loc,)),
            pltpu.SemaphoreType.DMA((3, 2)),
            pltpu.SemaphoreType.DMA((3, n_g)),
            pltpu.SemaphoreType.DMA((3, n_g)),
            pltpu.SemaphoreType.DMA((2, n_s)),
            pltpu.SemaphoreType.DMA((2, n_s)),
            pltpu.SemaphoreType.DMA((2,)),
            pltpu.SemaphoreType.DMA((2, n_tile)),
            pltpu.SemaphoreType.REGULAR,
            pltpu.SemaphoreType.DMA((d // tile_rows + 2, 2 * e_loc)),
            pltpu.SemaphoreType.DMA((n_peer,)),
            pltpu.SemaphoreType.DMA((n_peer,)),
        ],
        compiler_params=pltpu.CompilerParams(collective_id=0, has_side_effects=True, vmem_limit_bytes=67043328),
        name="moe",
    )(h_ext, dy, x_in, gain, bias, sel, sel_t, w_rt, pick, w_gate, w_up, w_down)


def solution(mesh):
    tok_spec = P(("dp", "ep", "tp"), None)
    wide_spec = P("ep", None, "tp")
    down_spec = P("ep", "tp", None)
    grad_wide = P(("dp", "ep"), None, "tp")
    grad_down = P(("dp", "ep"), "tp", None)
    side = mesh.shape["tp"]
    assert mesh.shape["ep"] == side * CORES

    def device_step(x_in, norm_gain, w_router, expert_idx, w_gate, w_up, w_down, out_bias, dy_out):
        n_tok, d_model = x_in.shape
        n_exp = w_router.shape[1]
        local_exp, _, ff = w_gate.shape
        n_ep = n_exp // local_exp
        x_f32 = x_in.astype(F32)
        inv_rms = lax.rsqrt(jnp.mean(x_f32 * x_f32, axis=-1, keepdims=True) + EPS)
        hidden = (x_f32 * inv_rms * norm_gain.astype(F32)).astype(BF16)
        logits = jnp.dot(hidden, w_router, preferred_element_type=F32)
        chosen = expert_idx[:, :, None] == jnp.arange(n_exp)[None, None, :]
        mask = jnp.any(chosen, axis=1)
        top = jnp.max(jnp.where(mask, logits, -jnp.inf), axis=-1, keepdims=True)
        unnorm = jnp.where(mask, jnp.exp(jnp.minimum(logits - top, 0.0)), 0.0)
        gates = unnorm / jnp.sum(unnorm, axis=-1, keepdims=True)
        hi = lax.reduce_precision(gates, 8, 7)
        mid = lax.reduce_precision(gates - hi, 8, 7)
        lo = gates - hi - mid
        zeros = jnp.zeros((n_tok, 128 - 3 * n_exp), F32)
        h_ext = jnp.concatenate([hidden, jnp.concatenate([hi, mid, lo, zeros], axis=1).astype(BF16)], axis=1)
        ep = lax.axis_index("ep")
        lane = jnp.arange(128)
        lane_e = jnp.where(lane < 3 * n_exp, lane % n_exp, n_exp)
        sel = (lane_e[:, None] == (ep * local_exp + jnp.arange(local_exp * ff) // ff)[None, :]).astype(BF16)
        slot = jnp.arange(n_ep * 8)
        slot_e = jnp.where(slot % 8 < local_exp, slot // 8 * local_exp + slot % 8, n_exp + 1)
        sel_t = (slot_e[:, None] == lane_e[None, :]).astype(BF16)
        pick = (jnp.arange(n_exp)[:, None] == slot_e[None, :]).astype(F32)
        w_rt = jnp.pad(w_router.T.reshape(n_ep, local_exp, d_model), ((0, 0), (0, 8 - local_exp), (0, 0))).reshape(n_ep * 8, d_model)
        row = lambda v: v.reshape(1, d_model)
        y_out, dx_in, d_gain, d_bias, d_router_t, d_gate, d_up, d_down = moe(mesh, h_ext, dy_out, x_in, row(norm_gain), row(out_bias), sel, sel_t, w_rt, pick, w_gate, w_up, w_down)
        return y_out, dx_in, d_gain.reshape(d_model), d_router_t.T, d_gate, d_up, d_down, d_bias.reshape(d_model)

    return jax.shard_map(device_step, mesh=mesh, in_specs=(tok_spec, P(None), P(None, None), tok_spec, wide_spec, wide_spec, down_spec, P(None), tok_spec), out_specs=(tok_spec, tok_spec, P("dp"), P("dp", None), grad_wide, grad_wide, grad_down, P("dp")), check_vma=False)
```

```python
import functools

import jax
import jax.numpy as jnp
from jax import lax
from jax.experimental import pallas as pl
from jax.experimental.pallas import tpu as pltpu
from jax.sharding import PartitionSpec as P

EPS = 1e-6
CORES = 2
BF16, F32 = jnp.bfloat16, jnp.float32
MESH = pl.DeviceIdType.MESH
NT = (((1,), (1,)), ((), ()))
TN = (((0,), (0,)), ((), ()))


def rows(start, size):
    return pl.ds(pl.multiple_of(start, size & -size), size)


class Place:
    def __init__(self, side):
        ep = lax.axis_index("ep")
        self.side = side
        self.x, self.c, self.y = lax.div(ep, CORES), lax.rem(ep, CORES), lax.axis_index("tp")

    def along(self, axis, step):
        if axis == "x":
            return {"ep": lax.rem(self.x + step + self.side, self.side) * CORES + self.c, "tp": self.y}
        return {"ep": self.x * CORES + self.c, "tp": lax.rem(self.y + step + self.side, self.side)}

    def partner(self):
        return {"ep": self.x * CORES + 1 - self.c, "tp": self.y}


class Half:
    def __init__(self, place, which, blk):
        self.p, self.which, self.blk, n = place, which, blk, place.side
        self.base = which * n
        self.major, self.minor = ("x", "y") if which == 0 else ("y", "x")
        self.m, self.n = (place.x, place.y) if which == 0 else (place.y, place.x)
        self.span = n * blk

    def tile(self, step):
        return self.base + lax.rem(self.m + step + self.p.side, self.p.side)

    def mine(self, part=0, parts=1):
        size = self.span // parts
        return rows(self.p.c * self.span + part * size, size)

    def block(self, step, part=0, parts=1):
        size = self.blk // parts
        return rows(self.p.c * self.span + lax.rem(self.n + step + self.p.side, self.p.side) * self.blk + part * size, size)


class Gather:
    COPIES = 17

    def __init__(self, halves, own, buf, send, recv):
        self.halves, self.own, self.buf, self.send, self.recv = halves, own, buf, send, recv

    def copy(self, h, k, src, dst, target):
        i = h.which * self.COPIES + k
        return pltpu.make_async_remote_copy(src_ref=src, dst_ref=dst, send_sem=self.send.at[i], recv_sem=self.recv.at[i], device_id=target, device_id_type=MESH)

    def make(self, h, k):
        b, p = self.buf, h.p
        same = lambda t, r, target: self.copy(h, k, b.at[t, r], b.at[t, r], target)
        s, d = 1 - 2 * (k % 2), k % 2
        if k < 2:
            return self.copy(h, k, self.own.at[pl.ds(h.which * h.blk, h.blk)], b.at[h.tile(0), h.block(0)], p.along(h.minor, s))
        if k < 4:
            return same(h.tile(0), h.block(-s, d, 2), p.along(h.minor, s))
        if k < 6:
            return same(h.tile(0), h.mine(d, 2), p.along(h.major, s))
        if k < 8:
            return same(h.tile(0), h.mine(1 - d, 2), p.along(h.major, s))
        if k < 10:
            return same(h.tile(-s), h.mine(d, 2), p.along(h.major, s))
        if k == 10:
            return same(h.tile(0), h.mine(), p.partner())
        step, part = ((-1, 0), (1, 1), (-1, 1), (1, 0), (2, 0), (2, 1))[k - 11]
        return same(h.tile(step), h.mine(part, 2), p.partner())

    def own_copy(self, h, sem):
        return pltpu.make_async_copy(self.own.at[pl.ds(h.which * h.blk, h.blk)], self.buf.at[h.tile(0), h.block(0)], sem)

    def start(self, *ks):
        for k in ks:
            for h in self.halves:
                self.make(h, k).start()

    def wait(self, *ks):
        for k in ks:
            for h in self.halves:
                self.make(h, k).wait_recv()

    def finish(self):
        for k in range(self.COPIES):
            for h in self.halves:
                self.make(h, k).wait_send()

    def begin(self, local):
        self.start(0, 1)
        for h in self.halves:
            self.own_copy(h, local.at[h.which]).start()

    def relay_minor(self, local):
        for h in self.halves:
            self.own_copy(h, local.at[h.which]).wait()
        self.wait(0, 1)
        self.start(2, 3)

    def share_own(self):
        self.wait(2, 3)
        self.start(10)

    def send_major(self):
        self.start(4, 5, 6, 7)

    def relay_major(self):
        self.wait(4, 5)
        self.start(8, 9, 11, 12)

    def share_near(self):
        self.wait(6, 7)
        self.start(13, 14)

    def share_far(self):
        self.wait(8, 9)
        self.start(15, 16)


class Scatter:
    COPIES = 12

    def __init__(self, halves, part, big, small, send, recv):
        self.halves, self.part, self.big, self.small, self.send, self.recv = halves, part, big, small, send, recv

    def piece(self, h, part, parts=2):
        size = h.span // parts
        return pl.ds(part * size, size)

    def block(self, h, step, part=0, parts=1):
        size = h.blk // parts
        return rows(lax.rem(h.n + step + h.p.side, h.p.side) * h.blk + part * size, size)

    def add(self, t, r, *terms):
        total = self.part[t, r].astype(F32)
        for term in terms:
            total = total + term.astype(F32)
        self.part[t, r] = total.astype(BF16)

    def land(self, h, k):
        if k < 6:
            return self.big.at[h.which, pl.ds(k * (h.span // 2), h.span // 2)]
        return self.small.at[h.which, pl.ds((k - 6) * (h.blk // 2), h.blk // 2)]

    def make(self, h, k):
        s, d = 1 - 2 * (k % 2), k % 2
        if k < 2:
            src = self.part.at[h.tile(2), self.piece(h, d)]
        elif k < 4:
            src = self.part.at[h.tile(s), self.piece(h, 1 - d)]
        elif k < 6:
            src = self.part.at[h.tile(s), self.piece(h, d)]
        elif k < 8:
            src = self.part.at[h.tile(0), self.block(h, 2, d, 2)]
        elif k < 10:
            src = self.part.at[h.tile(0), self.block(h, s, 1 - d, 2)]
        else:
            src = self.part.at[h.tile(0), self.block(h, s, d, 2)]
        i = h.which * self.COPIES + k
        axis = h.major if k < 6 else h.minor
        return pltpu.make_async_remote_copy(src_ref=src, dst_ref=self.land(h, k), send_sem=self.send.at[i], recv_sem=self.recv.at[i], device_id=h.p.along(axis, s), device_id_type=MESH)

    def start(self, h, *ks):
        for k in ks:
            self.make(h, k).start()

    def got(self, h, k):
        self.make(h, k).wait_recv()
        return self.land(h, k)[...]

    def begin_far(self):
        for h in self.halves:
            self.start(h, 0, 1)

    def begin_near(self):
        for h in self.halves:
            self.start(h, 2, 3)

    def begin(self):
        self.begin_far()
        self.begin_near()

    def relay_major(self):
        for h in self.halves:
            for d in (0, 1):
                self.add(h.tile(1 - 2 * d), self.piece(h, d), self.got(h, d))
                self.start(h, 4 + d)

    def turn(self):
        for h in self.halves:
            self.add(h.tile(0), self.piece(h, 0), self.got(h, 3), self.got(h, 4))
            self.add(h.tile(0), self.piece(h, 1), self.got(h, 2), self.got(h, 5))
            self.start(h, 6, 7, 8, 9)

    def relay_minor(self):
        for h in self.halves:
            for d in (0, 1):
                self.add(h.tile(0), self.block(h, 1 - 2 * d, d, 2), self.got(h, 6 + d))
                self.start(h, 10 + d)

    def total(self, h):
        mine = self.part[h.tile(0), self.block(h, 0)].astype(F32)
        low = self.got(h, 9).astype(F32) + self.got(h, 10).astype(F32)
        high = self.got(h, 8).astype(F32) + self.got(h, 11).astype(F32)
        return mine + jnp.concatenate([low, high], axis=0)

    def finish(self):
        for h in self.halves:
            for k in range(self.COPIES):
                self.make(h, k).wait_send()


def moe_kernel(side, d, e_loc, ff, n_exp, dy_in, x_ref, gain_ref, bias_ref, w_r, idx_ref, wg_hbm, wu_hbm, wd_hbm,
               y_ref, dx_ref, d_gain, d_bias, d_router_t, dwg_hbm, dwu_hbm, dwd_hbm,
               hid, dys, dgs, dg_own, w_gu, w_d, gated, d_gu, part_y, part_dh, stage, swap, big_y, big_dh, small_y, small_dh,
               gu, gx_s, da_s, wd_s, bias_s, dl_s, dr_s, ar1, ar2, h_in, sel, sel_t, w_rt,
               w_sem, local, g_send, g_recv, s_send, s_recv, stage_send, swap_recv, credit, out_sem, ar_send, ar_recv):
    place = Place(side)
    n_tile = 2 * side
    n_ep = side * CORES
    n_tok = x_ref.shape[0]
    blk = n_tok // 2
    halves = [Half(place, 0, blk), Half(place, 1, blk)]
    tile_rows = hid.shape[1]
    span = tile_rows // CORES
    mine, theirs = rows(place.c * span, span), rows((1 - place.c) * span, span)
    me_ep = lax.axis_index("ep")

    weights = []
    for e in range(e_loc):
        weights.append(pltpu.make_async_copy(wg_hbm.at[e], w_gu.at[:, pl.ds(2 * e * ff, ff)], w_sem.at[3 * e]))
        weights.append(pltpu.make_async_copy(wu_hbm.at[e], w_gu.at[:, pl.ds((2 * e + 1) * ff, ff)], w_sem.at[3 * e + 1]))
        weights.append(pltpu.make_async_copy(wd_hbm.at[e], w_d.at[pl.ds(e * ff, ff)], w_sem.at[3 * e + 2]))

    ep_peers = [{"ep": lax.rem(me_ep + o, n_ep), "tp": place.y} for o in range(1, n_ep)]
    tp_peers = [{"ep": me_ep, "tp": lax.rem(place.y + o, side)} for o in range(1, side)]
    barrier = pltpu.get_barrier_semaphore()
    for peer in ep_peers + tp_peers:
        pl.semaphore_signal(barrier, inc=1, device_id=peer, device_id_type=MESH)
    for w in weights:
        w.start()

    def lane_expert(shape, axis):
        at = lax.broadcasted_iota(jnp.int32, shape, axis)
        at = jnp.where(at >= 2 * n_exp, at - 2 * n_exp, jnp.where(at >= n_exp, at - n_exp, at))
        return jnp.where(at < n_exp, at, n_exp)

    def slot_expert(shape, axis):
        at = lax.broadcasted_iota(jnp.int32, shape, axis)
        low = jnp.bitwise_and(at, 7)
        return jnp.where(low < e_loc, jnp.right_shift(at, 3) * e_loc + low, n_exp + 1)

    def one_hot(cond, dtype=BF16):
        return jnp.where(cond, 1.0, 0.0).astype(dtype)

    def expert_row(shape):
        return lax.broadcasted_iota(jnp.int32, shape, 0)

    row_f32 = lambda ref: ref[...].astype(F32).reshape(1, d)
    x_f32 = x_ref[...].astype(F32)
    hidden = (x_f32 * lax.rsqrt(jnp.mean(x_f32 * x_f32, axis=1, keepdims=True) + EPS) * row_f32(gain_ref)).astype(BF16)
    h_in[:, pl.ds(0, d)] = hidden
    w_rep = lax.dot_general(one_hot(expert_row((n_exp, 128)) == lane_expert((n_exp, 128), 1)), w_r[...], TN, preferred_element_type=F32)
    logits = lax.dot_general(hidden, w_rep.astype(BF16), NT, preferred_element_type=F32)
    tok_expert = lane_expert((n_tok, 128), 1)
    chosen = idx_ref[:, 0:1] == tok_expert
    for j in range(1, idx_ref.shape[1]):
        chosen = jnp.logical_or(chosen, idx_ref[:, j:j + 1] == tok_expert)
    top = jnp.max(jnp.where(chosen, logits, -jnp.inf), axis=1, keepdims=True)
    unnorm = jnp.where(chosen, jnp.exp(jnp.minimum(logits - top, 0.0)), 0.0)
    tok_lane = lax.broadcasted_iota(jnp.int32, (n_tok, 128), 1)
    gates = unnorm / jnp.sum(jnp.where(tok_lane < n_exp, unnorm, 0.0), axis=1, keepdims=True)
    hi = gates.astype(BF16).astype(F32)
    mid = (gates - hi).astype(BF16).astype(F32)
    h_in[:, pl.ds(d, 128)] = jnp.where(tok_lane < n_exp, hi, jnp.where(tok_lane < 2 * n_exp, mid, gates - hi - mid)).astype(BF16)
    pl.semaphore_wait(barrier, n_ep + side - 2)

    gather_h = Gather(halves, h_in, hid, g_send.at[0], g_recv.at[0])
    gather_dy = Gather(halves, dy_in, dys, g_send.at[1], g_recv.at[1])
    gather_dg = Gather(halves, dg_own, dgs, g_send.at[2], g_recv.at[2])
    scat_y = Scatter(halves, part_y, big_y, small_y, s_send.at[0], s_recv.at[0])
    scat_dh = Scatter(halves, part_dh, big_dh, small_dh, s_send.at[1], s_recv.at[1])

    gather_h.begin(local.at[0])
    gather_dy.begin(local.at[1])
    for e in range(e_loc):
        sel[:, pl.ds(e * ff, ff)] = one_hot(lane_expert((128, ff), 0) == me_ep * e_loc + e)
    sel_t[...] = one_hot(slot_expert(sel_t.shape, 0) == lane_expert(sel_t.shape, 1))
    pick = slot_expert((n_exp, 8 * n_ep), 1) == expert_row((n_exp, 8 * n_ep))
    w_rt[...] = lax.dot_general(one_hot(pick), w_r[...], TN, preferred_element_type=F32).astype(BF16)
    gather_h.relay_minor(local.at[0])
    gather_dy.relay_minor(local.at[1])
    gather_h.share_own()
    gather_h.send_major()
    for w in weights:
        w.wait()

    lane = lax.broadcasted_iota(jnp.int32, (tile_rows, 128), 1)

    def index_of(s):
        back = lax.div(s, n_tile)
        i = s * (1 - back) + (2 * n_tile - 1 - s) * back
        j, which = lax.div(i, 2), lax.rem(i, 2)
        off = j + lax.div(j, 2) - 2 * lax.div(j, 3)
        return which * side + lax.rem(place.x * (1 - which) + place.y * which + off, side)

    def is_back(s):
        return s >= n_tile

    def swap_copy(s, kind, t):
        slot = lax.rem(s, 2)
        return pltpu.make_async_remote_copy(src_ref=stage.at[slot, theirs], dst_ref=swap.at[t], send_sem=stage_send.at[slot], recv_sem=swap_recv.at[kind, t], device_id=place.partner(), device_id_type=MESH)

    def settle(s):
        t = index_of(s)

        def take(kind, part):
            swap_copy(s, kind, t).wait_recv()
            part[t] = (part[t].astype(F32) + swap[t].astype(F32)).astype(BF16)

        @pl.when(jnp.logical_not(is_back(s)))
        def _():
            take(0, part_y)
            pl.semaphore_signal(credit, inc=1, device_id=place.partner(), device_id_type=MESH)

        @pl.when(is_back(s))
        def _():
            take(1, part_dh)

    def after(s, k, *actions):
        @pl.when(s == k)
        def _():
            for action in actions:
                action()

    def hand_over(s, kind, t, part, value):
        @pl.when(s >= 1)
        def _():
            settle(s - 1)

        if kind == 1:
            after(s, n_tile, scat_y.begin)
            after(s, n_tile + 2, scat_dh.begin_far)
            after(s, n_tile + 6, scat_dh.begin_near)

        @pl.when(s >= 2)
        def _():
            swap_copy(s, kind, t).wait_send()

        slot = lax.rem(s, 2)
        stage[slot] = value().astype(BF16)
        part[t] = stage[slot, mine]
        if kind == 1:
            @pl.when(s == n_tile)
            def _():
                pl.semaphore_wait(credit, n_tile)
        swap_copy(s, kind, t).start()

    def tile_step(s, _):
        t = index_of(s)

        after(s, 0, lambda: gather_h.wait(10))
        after(s, 1, gather_dy.share_own)
        after(s, 2, gather_h.relay_major, gather_dy.send_major, gather_h.share_near, lambda: gather_h.wait(11, 12, 13, 14))
        after(s, 5, gather_h.share_far)
        after(s, 6, gather_dy.relay_major, lambda: gather_h.wait(15, 16))
        after(s, 7, gather_dy.share_near)
        after(s, 8, gather_dy.share_far, lambda: gather_dy.wait(15, 16))
        after(s, 10, lambda: gather_dy.wait(11, 12, 13, 14))
        after(s, 11, scat_y.relay_major)
        after(s, 14, scat_y.turn, lambda: gather_dy.wait(10))

        @pl.when(jnp.logical_not(is_back(s)))
        def _():
            gu[t] = jnp.dot(hid[t, :, pl.ds(0, d)], w_gu[...], preferred_element_type=F32)
            gx_s[...] = jnp.dot(hid[t, :, pl.ds(d, 128)], sel[...], preferred_element_type=F32)
            for e in range(e_loc):
                pre, up = gu[t, :, pl.ds(2 * e * ff, ff)], gu[t, :, pl.ds((2 * e + 1) * ff, ff)]
                act = pre * jax.nn.sigmoid(pre) * up
                gated[t, :, pl.ds(e * ff, ff)] = (act * gx_s[:, pl.ds(e * ff, ff)]).astype(BF16)
            hand_over(s, 0, t, part_y, lambda: jnp.dot(gated[t], w_d[...], preferred_element_type=F32))

        @pl.when(is_back(s))
        def _():
            gx_s[...] = jnp.dot(hid[t, :, pl.ds(d, 128)], sel[...], preferred_element_type=F32)
            da_s[...] = lax.dot_general(dys[t], w_d[...], NT, preferred_element_type=F32)
            bias_s[t] = jnp.sum(dys[t].astype(F32), axis=0, keepdims=True)
            sums = jnp.zeros((tile_rows, 128), F32)
            for e in range(e_loc):
                pre, up = gu[t, :, pl.ds(2 * e * ff, ff)], gu[t, :, pl.ds((2 * e + 1) * ff, ff)]
                gate, da = gx_s[:, pl.ds(e * ff, ff)], da_s[:, pl.ds(e * ff, ff)]
                sigma = jax.nn.sigmoid(pre)
                silu = pre * sigma
                sums = sums + jnp.where(lane == e, jnp.sum(silu * up * da, axis=1, keepdims=True), 0.0)
                da = da * gate
                d_gu[t, :, pl.ds(2 * e * ff, ff)] = (da * up * sigma * (1.0 + pre * (1.0 - sigma))).astype(BF16)
                d_gu[t, :, pl.ds((2 * e + 1) * ff, ff)] = (da * silu).astype(BF16)
            dg_own[rows(t * 8, 8)] = jnp.transpose(sums)[:8]
            hand_over(s, 1, t, part_dh, lambda: lax.dot_general(d_gu[t], w_gu[...], NT, preferred_element_type=F32))

        return 0

    steps = 2 * n_tile
    lax.fori_loop(0, steps, tile_step, 0)

    gather_dg.begin(local.at[2])
    settle(steps - 1)
    scat_dh.relay_major()
    scat_y.relay_minor()
    d_bias[...] = jnp.sum(bias_s[...], axis=0)

    m_blk = tile_rows
    n_m = d // m_blk

    def wide_copies(mb):
        out = []
        for e in range(e_loc):
            for j, ref in enumerate((dwg_hbm, dwu_hbm)):
                out.append(pltpu.make_async_copy(gu.at[mb, :, pl.ds((2 * e + j) * ff, ff)], ref.at[e, rows(mb * m_blk, m_blk)], out_sem.at[mb, 2 * e + j]))
        return out

    def wide_step(mb, _):
        a = hid[:, :, rows(mb * m_blk, m_blk)].reshape(n_tile * tile_rows, m_blk)
        b = d_gu[...].reshape(n_tile * tile_rows, 2 * e_loc * ff)
        gu[mb] = lax.dot_general(a, b, TN, preferred_element_type=F32)
        for cp in wide_copies(mb):
            cp.start()

        after(mb, 0, lambda: gather_dg.relay_minor(local.at[2]))
        after(mb, 1, gather_dg.share_own, gather_dg.send_major)
        after(mb, 3, scat_dh.turn)
        after(mb, 4, gather_dg.relay_major)
        after(mb, 5, scat_dh.relay_minor, gather_dg.share_near)
        return 0

    lax.fori_loop(0, n_m, wide_step, 0)

    for h in halves:
        r = pl.ds(h.which * blk, blk)
        y_ref[r] = (x_ref[r].astype(F32) + scat_y.total(h) + row_f32(bias_ref)).astype(BF16)

    n_blk = wd_s.shape[2]
    n_n = d // n_blk

    def down_copies(nb):
        slot = lax.rem(nb, 2)
        return [pltpu.make_async_copy(wd_s.at[slot, pl.ds(e * ff, ff)], dwd_hbm.at[e, :, rows(nb * n_blk, n_blk)], out_sem.at[n_m + slot, e]) for e in range(e_loc)]

    def down_step(nb, _):
        @pl.when(nb > 1)
        def _():
            for cp in down_copies(nb - 2):
                cp.wait()
        a = gated[...].reshape(n_tile * tile_rows, e_loc * ff)
        b = dys[:, :, rows(nb * n_blk, n_blk)].reshape(n_tile * tile_rows, n_blk)
        wd_s[lax.rem(nb, 2)] = lax.dot_general(a, b, TN, preferred_element_type=F32)
        for cp in down_copies(nb):
            cp.start()

        after(nb, 0, gather_dg.share_far)
        return 0

    lax.fori_loop(0, n_n, down_step, 0)

    gather_dg.wait(10, 11, 12, 13, 14, 15, 16)
    dr_s[...] = jnp.zeros_like(dr_s)
    for t in range(n_tile):
        which, tl = t // side, t % side
        pieces = []
        for ep in range(n_ep):
            px, pc = ep // CORES, ep % CORES
            total = None
            for py in range(side):
                if which == 0:
                    term = dgs[px, pl.ds((pc * side + py) * blk + tl * 8, 8)]
                else:
                    term = dgs[side + py, pl.ds((pc * side + px) * blk + tl * 8, 8)]
                total = term if total is None else total + term
            pieces.append(total)
        d_g = jnp.concatenate(pieces, axis=0)
        g_t = lax.dot_general(sel_t[...], hid[t, :, pl.ds(d, 128)], NT, preferred_element_type=F32)
        d_l = (g_t * (d_g - jnp.sum(g_t * d_g, axis=0, keepdims=True))).astype(BF16)
        dl_s[t] = d_l
        dr_s[...] += jnp.dot(d_l, hid[t, :, pl.ds(0, d)], preferred_element_type=F32)
    d_router_t[...] = jnp.dot(one_hot(pick, F32), dr_s[...], preferred_element_type=F32, precision=lax.Precision.HIGHEST)

    gain = row_f32(gain_ref)
    gain_part = jnp.zeros((1, d), F32)
    for h in halves:
        r = pl.ds(h.which * blk, blk)
        routed = lax.dot_general(dl_s[h.tile(0), :, mine], w_rt[...], TN, preferred_element_type=F32)
        own = jnp.zeros((blk, d), F32)
        for q in range(side):
            own = own + jnp.where(h.n == q, routed[q * blk:(q + 1) * blk], 0.0)
        x_f32 = x_ref[r].astype(F32)
        inv_rms = lax.rsqrt(jnp.mean(x_f32 * x_f32, axis=1, keepdims=True) + EPS)
        normed = x_f32 * inv_rms
        dh = scat_dh.total(h) + own
        gain_part = gain_part + jnp.sum(dh * normed, axis=0, keepdims=True)
        d_norm = dh * gain
        dx_ref[r] = (dy_in[r].astype(F32) + inv_rms * (d_norm - normed * jnp.mean(d_norm * normed, axis=1, keepdims=True))).astype(BF16)

    def spread(buf, slot, peers, first):
        out = []
        for o, peer in enumerate(peers):
            out.append(pltpu.make_async_remote_copy(src_ref=buf.at[slot], dst_ref=buf.at[slot], send_sem=ar_send.at[first + o], recv_sem=ar_recv.at[first + o], device_id=peer, device_id_type=MESH))
        for cp in out:
            cp.start()
        for cp in out:
            cp.wait_recv()
        return out

    ar1[me_ep] = gain_part
    sent = spread(ar1, me_ep, ep_peers, 0)
    ar2[place.y] = jnp.sum(ar1[...], axis=0)
    sent += spread(ar2, place.y, tp_peers, n_ep - 1)
    d_gain[...] = jnp.sum(ar2[...], axis=0)

    for cp in sent:
        cp.wait_send()
    for g in (gather_h, gather_dy, gather_dg):
        g.finish()
    for sc in (scat_y, scat_dh):
        sc.finish()
    for s in (steps - 2, steps - 1):
        swap_copy(s, 1, index_of(s)).wait_send()
    for mb in range(n_m):
        for cp in wide_copies(mb):
            cp.wait()
    for nb in (n_n - 2, n_n - 1):
        for cp in down_copies(nb):
            cp.wait()


def moe(mesh, dy, x_in, gain, bias, w_r, idx, w_gate, w_up, w_down):
    side = mesh.shape["tp"]
    n_tok, d = dy.shape
    e_loc, _, ff = w_gate.shape
    tile_rows = CORES * side * n_tok // 2
    span = tile_rows // CORES
    n_tile = 2 * side
    n_ep = side * CORES
    n_exp = n_ep * e_loc
    dx = d + 128
    vm = pl.BlockSpec(memory_space=pltpu.VMEM)
    hbm = pl.BlockSpec(memory_space=pl.ANY)
    blk = n_tok // 2
    n_g, n_s = 2 * Gather.COPIES, 2 * Scatter.COPIES
    n_peer = n_ep + side - 2
    return pl.pallas_call(
        functools.partial(moe_kernel, side, d, e_loc, ff, n_exp),
        out_shape=(
            jax.ShapeDtypeStruct((n_tok, d), BF16),
            jax.ShapeDtypeStruct((n_tok, d), BF16),
            jax.ShapeDtypeStruct((1, d), F32),
            jax.ShapeDtypeStruct((1, d), F32),
            jax.ShapeDtypeStruct((n_exp, d), F32),
            jax.ShapeDtypeStruct(w_gate.shape, F32),
            jax.ShapeDtypeStruct(w_up.shape, F32),
            jax.ShapeDtypeStruct(w_down.shape, F32),
        ),
        in_specs=[vm] * 6 + [hbm] * 3,
        out_specs=(vm, vm, vm, vm, vm, hbm, hbm, hbm),
        scratch_shapes=[
            pltpu.VMEM((n_tile, tile_rows, dx), BF16),
            pltpu.VMEM((n_tile, tile_rows, d), BF16),
            pltpu.VMEM((n_tile, tile_rows, tile_rows), F32),
            pltpu.VMEM((n_tok, tile_rows), F32),
            pltpu.VMEM((d, 2 * e_loc * ff), BF16),
            pltpu.VMEM((e_loc * ff, d), BF16),
            pltpu.VMEM((n_tile, tile_rows, e_loc * ff), BF16),
            pltpu.VMEM((n_tile, tile_rows, 2 * e_loc * ff), BF16),
            pltpu.VMEM((n_tile, span, d), BF16),
            pltpu.VMEM((n_tile, span, d), BF16),
            pltpu.VMEM((2, tile_rows, d), BF16),
            pltpu.VMEM((n_tile, span, d), BF16),
            pltpu.VMEM((2, 3 * span, d), BF16),
            pltpu.VMEM((2, 3 * span, d), BF16),
            pltpu.VMEM((2, 3 * blk, d), BF16),
            pltpu.VMEM((2, 3 * blk, d), BF16),
            pltpu.VMEM((n_tile, tile_rows, 2 * e_loc * ff), F32),
            pltpu.VMEM((tile_rows, e_loc * ff), F32),
            pltpu.VMEM((tile_rows, e_loc * ff), F32),
            pltpu.VMEM((2, e_loc * ff, 256), F32),
            pltpu.VMEM((n_tile, 1, d), F32),
            pltpu.VMEM((n_tile, n_ep * 8, tile_rows), BF16),
            pltpu.VMEM((n_ep * 8, d), F32),
            pltpu.VMEM((n_ep, 1, d), F32),
            pltpu.VMEM((side, 1, d), F32),
            pltpu.VMEM((n_tok, dx), BF16),
            pltpu.VMEM((128, e_loc * ff), BF16),
            pltpu.VMEM((n_ep * 8, 128), BF16),
            pltpu.VMEM((n_ep * 8, d), BF16),
            pltpu.SemaphoreType.DMA((3 * e_loc,)),
            pltpu.SemaphoreType.DMA((3, 2)),
            pltpu.SemaphoreType.DMA((3, n_g)),
            pltpu.SemaphoreType.DMA((3, n_g)),
            pltpu.SemaphoreType.DMA((2, n_s)),
            pltpu.SemaphoreType.DMA((2, n_s)),
            pltpu.SemaphoreType.DMA((2,)),
            pltpu.SemaphoreType.DMA((2, n_tile)),
            pltpu.SemaphoreType.REGULAR,
            pltpu.SemaphoreType.DMA((d // tile_rows + 2, 2 * e_loc)),
            pltpu.SemaphoreType.DMA((n_peer,)),
            pltpu.SemaphoreType.DMA((n_peer,)),
        ],
        compiler_params=pltpu.CompilerParams(collective_id=0, has_side_effects=True, vmem_limit_bytes=67043328),
        name="moe",
    )(dy, x_in, gain, bias, w_r, idx, w_gate, w_up, w_down)


def solution(mesh):
    tok_spec = P(("dp", "ep", "tp"), None)
    wide_spec = P("ep", None, "tp")
    down_spec = P("ep", "tp", None)
    grad_wide = P(("dp", "ep"), None, "tp")
    grad_down = P(("dp", "ep"), "tp", None)
    side = mesh.shape["tp"]
    assert mesh.shape["ep"] == side * CORES

    def device_step(x_in, norm_gain, w_router, expert_idx, w_gate, w_up, w_down, out_bias, dy_out):
        d_model = x_in.shape[1]
        y_out, dx_in, d_gain, d_bias, d_router_t, d_gate, d_up, d_down = moe(mesh, dy_out, x_in, norm_gain, out_bias, w_router.T, expert_idx, w_gate, w_up, w_down)
        return y_out, dx_in, d_gain.reshape(d_model), d_router_t.T, d_gate, d_up, d_down, d_bias.reshape(d_model)

    return jax.shard_map(device_step, mesh=mesh, in_specs=(tok_spec, P(None), P(None, None), tok_spec, wide_spec, wide_spec, down_spec, P(None), tok_spec), out_specs=(tok_spec, tok_spec, P("dp"), P("dp", None), grad_wide, grad_wide, grad_down, P("dp")), check_vma=False)
```

```python
import functools

import jax
import jax.numpy as jnp
from jax import lax
from jax.experimental import pallas as pl
from jax.experimental.pallas import tpu as pltpu
from jax.sharding import PartitionSpec as P

EPS = 1e-6
CORES = 2
BF16, F32 = jnp.bfloat16, jnp.float32
MESH = pl.DeviceIdType.MESH
NT = (((1,), (1,)), ((), ()))
TN = (((0,), (0,)), ((), ()))


def rows(start, size):
    return pl.ds(pl.multiple_of(start, size & -size), size)


class Place:
    def __init__(self, side):
        ep = lax.axis_index("ep")
        self.side = side
        self.x, self.c, self.y = lax.div(ep, CORES), lax.rem(ep, CORES), lax.axis_index("tp")

    def along(self, axis, step):
        if axis == "x":
            return {"ep": lax.rem(self.x + step + self.side, self.side) * CORES + self.c, "tp": self.y}
        return {"ep": self.x * CORES + self.c, "tp": lax.rem(self.y + step + self.side, self.side)}

    def partner(self):
        return {"ep": self.x * CORES + 1 - self.c, "tp": self.y}


class Half:
    def __init__(self, place, which, blk):
        self.p, self.which, self.blk, n = place, which, blk, place.side
        self.base = which * n
        self.major, self.minor = ("x", "y") if which == 0 else ("y", "x")
        self.m, self.n = (place.x, place.y) if which == 0 else (place.y, place.x)
        self.span = n * blk

    def tile(self, step):
        return self.base + lax.rem(self.m + step + self.p.side, self.p.side)

    def mine(self, part=0, parts=1):
        size = self.span // parts
        return rows(self.p.c * self.span + part * size, size)

    def block(self, step, part=0, parts=1):
        size = self.blk // parts
        return rows(self.p.c * self.span + lax.rem(self.n + step + self.p.side, self.p.side) * self.blk + part * size, size)


class Gather:
    COPIES = 20
    OFFSETS = (0, -1, 1, 2)

    def __init__(self, halves, own, buf, send, recv):
        self.halves, self.own, self.buf, self.send, self.recv = halves, own, buf, send, recv

    def copy(self, h, k, src, dst, target):
        i = h.which * self.COPIES + k
        return pltpu.make_async_remote_copy(src_ref=src, dst_ref=dst, send_sem=self.send.at[i], recv_sem=self.recv.at[i], device_id=target, device_id_type=MESH)

    def make(self, h, k):
        b, p = self.buf, h.p
        same = lambda t, r, target: self.copy(h, k, b.at[t, r], b.at[t, r], target)
        s, d = 1 - 2 * (k % 2), k % 2
        if k in (2, 3):
            return same(h.tile(0), h.block(-s, d, 2), p.along(h.minor, s))
        if k < 6:
            return self.copy(h, k, self.own.at[pl.ds(h.which * h.blk, h.blk)], b.at[h.tile(0), h.block(0)], p.along(h.minor if k < 2 else h.major, s))
        if k < 12:
            return same(h.tile(0), h.block(self.OFFSETS[(k - 4) // 2]), p.along(h.major, s))
        if k < 16:
            return same(h.tile(-s), h.block((0, 1, -1, 2)[k - 12]), p.along(h.major, s))
        return same(h.tile((0, -1, 1, 2)[k - 16]), h.mine(), p.partner())

    def own_copy(self, h, sem):
        return pltpu.make_async_copy(self.own.at[pl.ds(h.which * h.blk, h.blk)], self.buf.at[h.tile(0), h.block(0)], sem)

    def start(self, *ks):
        for k in ks:
            for h in self.halves:
                self.make(h, k).start()

    def wait(self, *ks):
        for k in ks:
            for h in self.halves:
                self.make(h, k).wait_recv()

    def finish(self):
        for k in range(self.COPIES):
            for h in self.halves:
                self.make(h, k).wait_send()

    def begin(self, local):
        self.start(0, 1, 4, 5)
        for h in self.halves:
            self.own_copy(h, local.at[h.which]).start()

    def relay_minor(self, local):
        for h in self.halves:
            self.own_copy(h, local.at[h.which]).wait()
        self.wait(0, 1)
        self.start(2, 3, 6, 7, 8, 9)
        self.wait(4)
        self.start(12)

    def share_own(self):
        self.wait(2, 3)
        self.start(10, 11, 16)

    def relay_major(self):
        self.wait(6)
        self.start(14)
        self.wait(9)
        self.start(13)

    def share_near(self):
        self.wait(11)
        self.start(15)
        self.wait(8, 10, 5, 7)
        self.start(17, 18)

    def share_far(self):
        self.wait(12, 13, 14, 15)
        self.start(19)


class Scatter:
    COPIES = 12

    def __init__(self, halves, part, big, small, send, recv):
        self.halves, self.part, self.big, self.small, self.send, self.recv = halves, part, big, small, send, recv

    def piece(self, h, part, parts=2):
        size = h.span // parts
        return pl.ds(part * size, size)

    def block(self, h, step, part=0, parts=1):
        size = h.blk // parts
        return rows(lax.rem(h.n + step + h.p.side, h.p.side) * h.blk + part * size, size)

    def add(self, t, r, *terms):
        total = self.part[t, r].astype(F32)
        for term in terms:
            total = total + term.astype(F32)
        self.part[t, r] = total.astype(BF16)

    def land(self, h, k):
        if k < 6:
            return self.big.at[h.which, pl.ds(k * (h.span // 2), h.span // 2)]
        return self.small.at[h.which, pl.ds((k - 6) * (h.blk // 2), h.blk // 2)]

    def make(self, h, k):
        s, d = 1 - 2 * (k % 2), k % 2
        if k < 2:
            src = self.part.at[h.tile(2), self.piece(h, d)]
        elif k < 4:
            src = self.part.at[h.tile(s), self.piece(h, 1 - d)]
        elif k < 6:
            src = self.part.at[h.tile(s), self.piece(h, d)]
        elif k < 8:
            src = self.part.at[h.tile(0), self.block(h, 2, d, 2)]
        elif k < 10:
            src = self.part.at[h.tile(0), self.block(h, s, 1 - d, 2)]
        else:
            src = self.part.at[h.tile(0), self.block(h, s, d, 2)]
        i = h.which * self.COPIES + k
        axis = h.major if k < 6 else h.minor
        return pltpu.make_async_remote_copy(src_ref=src, dst_ref=self.land(h, k), send_sem=self.send.at[i], recv_sem=self.recv.at[i], device_id=h.p.along(axis, s), device_id_type=MESH)

    def start(self, h, *ks):
        for k in ks:
            self.make(h, k).start()

    def got(self, h, k):
        self.make(h, k).wait_recv()
        return self.land(h, k)[...]

    def begin_far(self):
        for h in self.halves:
            self.start(h, 0, 1)

    def begin_near(self):
        for h in self.halves:
            self.start(h, 2, 3)

    def begin(self):
        self.begin_far()
        self.begin_near()

    def relay_major(self):
        for h in self.halves:
            for d in (0, 1):
                self.add(h.tile(1 - 2 * d), self.piece(h, d), self.got(h, d))
                self.start(h, 4 + d)

    def turn(self):
        for h in self.halves:
            self.add(h.tile(0), self.piece(h, 0), self.got(h, 3), self.got(h, 4))
            self.add(h.tile(0), self.piece(h, 1), self.got(h, 2), self.got(h, 5))
            self.start(h, 6, 7, 8, 9)

    def relay_minor(self):
        for h in self.halves:
            for d in (0, 1):
                self.add(h.tile(0), self.block(h, 1 - 2 * d, d, 2), self.got(h, 6 + d))
                self.start(h, 10 + d)

    def total(self, h):
        mine = self.part[h.tile(0), self.block(h, 0)].astype(F32)
        low = self.got(h, 9).astype(F32) + self.got(h, 10).astype(F32)
        high = self.got(h, 8).astype(F32) + self.got(h, 11).astype(F32)
        return mine + jnp.concatenate([low, high], axis=0)

    def finish(self):
        for h in self.halves:
            for k in range(self.COPIES):
                self.make(h, k).wait_send()


def moe_kernel(side, d, e_loc, ff, n_exp, dy_in, x_ref, gain_ref, bias_ref, w_r, idx_ref, wg_hbm, wu_hbm, wd_hbm,
               y_ref, dx_ref, d_gain, d_bias, d_router_t, dwg_hbm, dwu_hbm, dwd_hbm,
               hid, dys, dgs, dg_own, w_gu, w_d, gated, d_gu, part_y, part_dh, stage, swap, big_y, big_dh, small_y, small_dh,
               gu, gx_s, da_s, wd_s, bias_s, dl_s, dr_s, ar1, ar2, h_in, sel, sel_t, w_rt,
               w_sem, local, g_send, g_recv, s_send, s_recv, stage_send, swap_recv, credit, out_sem, ar_send, ar_recv):
    place = Place(side)
    n_tile = 2 * side
    n_ep = side * CORES
    n_tok = x_ref.shape[0]
    blk = n_tok // 2
    halves = [Half(place, 0, blk), Half(place, 1, blk)]
    tile_rows = hid.shape[1]
    span = tile_rows // CORES
    mine, theirs = rows(place.c * span, span), rows((1 - place.c) * span, span)
    me_ep = lax.axis_index("ep")

    weights = []
    for e in range(e_loc):
        weights.append(pltpu.make_async_copy(wg_hbm.at[e], w_gu.at[:, pl.ds(2 * e * ff, ff)], w_sem.at[3 * e]))
        weights.append(pltpu.make_async_copy(wu_hbm.at[e], w_gu.at[:, pl.ds((2 * e + 1) * ff, ff)], w_sem.at[3 * e + 1]))
        weights.append(pltpu.make_async_copy(wd_hbm.at[e], w_d.at[pl.ds(e * ff, ff)], w_sem.at[3 * e + 2]))

    ep_peers = [{"ep": lax.rem(me_ep + o, n_ep), "tp": place.y} for o in range(1, n_ep)]
    tp_peers = [{"ep": me_ep, "tp": lax.rem(place.y + o, side)} for o in range(1, side)]
    barrier = pltpu.get_barrier_semaphore()
    for peer in ep_peers + tp_peers:
        pl.semaphore_signal(barrier, inc=1, device_id=peer, device_id_type=MESH)
    for w in weights:
        w.start()

    def lane_expert(shape, axis):
        at = lax.broadcasted_iota(jnp.int32, shape, axis)
        at = jnp.where(at >= 2 * n_exp, at - 2 * n_exp, jnp.where(at >= n_exp, at - n_exp, at))
        return jnp.where(at < n_exp, at, n_exp)

    def slot_expert(shape, axis):
        at = lax.broadcasted_iota(jnp.int32, shape, axis)
        low = jnp.bitwise_and(at, 7)
        return jnp.where(low < e_loc, jnp.right_shift(at, 3) * e_loc + low, n_exp + 1)

    def one_hot(cond, dtype=BF16):
        return jnp.where(cond, 1.0, 0.0).astype(dtype)

    def expert_row(shape):
        return lax.broadcasted_iota(jnp.int32, shape, 0)

    row_f32 = lambda ref: ref[...].astype(F32).reshape(1, d)
    x_f32 = x_ref[...].astype(F32)
    hidden = (x_f32 * lax.rsqrt(jnp.mean(x_f32 * x_f32, axis=1, keepdims=True) + EPS) * row_f32(gain_ref)).astype(BF16)
    h_in[:, pl.ds(0, d)] = hidden
    w_rep = lax.dot_general(one_hot(expert_row((n_exp, 128)) == lane_expert((n_exp, 128), 1)), w_r[...], TN, preferred_element_type=F32)
    logits = lax.dot_general(hidden, w_rep.astype(BF16), NT, preferred_element_type=F32)
    tok_expert = lane_expert((n_tok, 128), 1)
    chosen = idx_ref[:, 0:1] == tok_expert
    for j in range(1, idx_ref.shape[1]):
        chosen = jnp.logical_or(chosen, idx_ref[:, j:j + 1] == tok_expert)
    top = jnp.max(jnp.where(chosen, logits, -jnp.inf), axis=1, keepdims=True)
    unnorm = jnp.where(chosen, jnp.exp(jnp.minimum(logits - top, 0.0)), 0.0)
    tok_lane = lax.broadcasted_iota(jnp.int32, (n_tok, 128), 1)
    gates = unnorm / jnp.sum(jnp.where(tok_lane < n_exp, unnorm, 0.0), axis=1, keepdims=True)
    hi = gates.astype(BF16).astype(F32)
    mid = (gates - hi).astype(BF16).astype(F32)
    h_in[:, pl.ds(d, 128)] = jnp.where(tok_lane < n_exp, hi, jnp.where(tok_lane < 2 * n_exp, mid, gates - hi - mid)).astype(BF16)
    pl.semaphore_wait(barrier, n_ep + side - 2)

    gather_h = Gather(halves, h_in, hid, g_send.at[0], g_recv.at[0])
    gather_dy = Gather(halves, dy_in, dys, g_send.at[1], g_recv.at[1])
    gather_dg = Gather(halves, dg_own, dgs, g_send.at[2], g_recv.at[2])
    scat_y = Scatter(halves, part_y, big_y, small_y, s_send.at[0], s_recv.at[0])
    scat_dh = Scatter(halves, part_dh, big_dh, small_dh, s_send.at[1], s_recv.at[1])

    gather_h.begin(local.at[0])
    gather_dy.begin(local.at[1])
    for e in range(e_loc):
        sel[:, pl.ds(e * ff, ff)] = one_hot(lane_expert((128, ff), 0) == me_ep * e_loc + e)
    sel_t[...] = one_hot(slot_expert(sel_t.shape, 0) == lane_expert(sel_t.shape, 1))
    pick = slot_expert((n_exp, 8 * n_ep), 1) == expert_row((n_exp, 8 * n_ep))
    w_rt[...] = lax.dot_general(one_hot(pick), w_r[...], TN, preferred_element_type=F32).astype(BF16)
    gather_h.relay_minor(local.at[0])
    gather_h.share_own()
    for w in weights:
        w.wait()

    lane = lax.broadcasted_iota(jnp.int32, (tile_rows, 128), 1)

    def index_of(s):
        back = lax.div(s, n_tile)
        r = s - n_tile
        late = lax.div(r, 2)
        j_back = jnp.where(late == 0, 1, jnp.where(late == 1, 3, jnp.where(late == 2, 2, 0)))
        i = jnp.where(back == 0, s, 2 * j_back + lax.rem(r, 2))
        j, which = lax.div(i, 2), lax.rem(i, 2)
        off = j + lax.div(j, 2) - 2 * lax.div(j, 3)
        return which * side + lax.rem(place.x * (1 - which) + place.y * which + off, side)

    def is_back(s):
        return s >= n_tile

    def swap_copy(s, kind, t):
        slot = lax.rem(s, 2)
        return pltpu.make_async_remote_copy(src_ref=stage.at[slot, theirs], dst_ref=swap.at[t], send_sem=stage_send.at[slot], recv_sem=swap_recv.at[kind, t], device_id=place.partner(), device_id_type=MESH)

    def settle(s):
        t = index_of(s)

        def take(kind, part):
            swap_copy(s, kind, t).wait_recv()
            part[t] = (part[t].astype(F32) + swap[t].astype(F32)).astype(BF16)

        @pl.when(jnp.logical_not(is_back(s)))
        def _():
            take(0, part_y)
            pl.semaphore_signal(credit, inc=1, device_id=place.partner(), device_id_type=MESH)

        @pl.when(is_back(s))
        def _():
            take(1, part_dh)

    def after(s, k, *actions):
        @pl.when(s == k)
        def _():
            for action in actions:
                action()

    def hand_over(s, kind, t, part, value):
        @pl.when(s >= 1)
        def _():
            settle(s - 1)

        if kind == 1:
            after(s, n_tile, scat_y.begin)
            after(s, n_tile + 4, scat_dh.begin_far)
            after(s, n_tile + 6, scat_dh.begin_near)

        @pl.when(s >= 2)
        def _():
            swap_copy(s, kind, t).wait_send()

        slot = lax.rem(s, 2)
        stage[slot] = value().astype(BF16)
        part[t] = stage[slot, mine]
        if kind == 1:
            @pl.when(s == n_tile)
            def _():
                pl.semaphore_wait(credit, n_tile)
        swap_copy(s, kind, t).start()

    def tile_step(s, _):
        t = index_of(s)

        after(s, 0, lambda: gather_h.wait(16))
        after(s, 1, gather_h.relay_major, lambda: gather_dy.relay_minor(local.at[1]))
        after(s, 2, gather_h.share_near, lambda: gather_h.wait(17, 18))
        after(s, 3, gather_dy.share_own)
        after(s, 4, gather_h.share_far, gather_dy.relay_major)
        after(s, 6, lambda: gather_h.wait(19), gather_dy.share_near)
        after(s, 8, gather_dy.share_far, lambda: gather_dy.wait(17, 18))
        after(s, 10, lambda: gather_dy.wait(19))
        after(s, 11, scat_y.relay_major)
        after(s, 13, scat_y.turn)
        after(s, 14, lambda: gather_dy.wait(16))
        after(s, 15, scat_dh.relay_major, scat_y.relay_minor)

        @pl.when(jnp.logical_not(is_back(s)))
        def _():
            gu[t] = jnp.dot(hid[t, :, pl.ds(0, d)], w_gu[...], preferred_element_type=F32)
            gx_s[...] = jnp.dot(hid[t, :, pl.ds(d, 128)], sel[...], preferred_element_type=F32)
            for e in range(e_loc):
                pre, up = gu[t, :, pl.ds(2 * e * ff, ff)], gu[t, :, pl.ds((2 * e + 1) * ff, ff)]
                act = pre * jax.nn.sigmoid(pre) * up
                gated[t, :, pl.ds(e * ff, ff)] = (act * gx_s[:, pl.ds(e * ff, ff)]).astype(BF16)
            hand_over(s, 0, t, part_y, lambda: jnp.dot(gated[t], w_d[...], preferred_element_type=F32))

        @pl.when(is_back(s))
        def _():
            gx_s[...] = jnp.dot(hid[t, :, pl.ds(d, 128)], sel[...], preferred_element_type=F32)
            da_s[...] = lax.dot_general(dys[t], w_d[...], NT, preferred_element_type=F32)
            bias_s[t] = jnp.sum(dys[t].astype(F32), axis=0, keepdims=True)
            sums = jnp.zeros((tile_rows, 128), F32)
            for e in range(e_loc):
                pre, up = gu[t, :, pl.ds(2 * e * ff, ff)], gu[t, :, pl.ds((2 * e + 1) * ff, ff)]
                gate, da = gx_s[:, pl.ds(e * ff, ff)], da_s[:, pl.ds(e * ff, ff)]
                sigma = jax.nn.sigmoid(pre)
                silu = pre * sigma
                sums = sums + jnp.where(lane == e, jnp.sum(silu * up * da, axis=1, keepdims=True), 0.0)
                da = da * gate
                d_gu[t, :, pl.ds(2 * e * ff, ff)] = (da * up * sigma * (1.0 + pre * (1.0 - sigma))).astype(BF16)
                d_gu[t, :, pl.ds((2 * e + 1) * ff, ff)] = (da * silu).astype(BF16)
            dg_own[rows(t * 8, 8)] = jnp.transpose(sums)[:8]
            hand_over(s, 1, t, part_dh, lambda: lax.dot_general(d_gu[t], w_gu[...], NT, preferred_element_type=F32))

        return 0

    steps = 2 * n_tile
    lax.fori_loop(0, steps, tile_step, 0)

    gather_dg.begin(local.at[2])
    settle(steps - 1)
    d_bias[...] = jnp.sum(bias_s[...], axis=0)

    m_blk = tile_rows
    n_m = d // m_blk

    def wide_copies(mb):
        out = []
        for e in range(e_loc):
            for j, ref in enumerate((dwg_hbm, dwu_hbm)):
                out.append(pltpu.make_async_copy(gu.at[mb, :, pl.ds((2 * e + j) * ff, ff)], ref.at[e, rows(mb * m_blk, m_blk)], out_sem.at[mb, 2 * e + j]))
        return out

    def wide_step(mb, _):
        a = hid[:, :, rows(mb * m_blk, m_blk)].reshape(n_tile * tile_rows, m_blk)
        b = d_gu[...].reshape(n_tile * tile_rows, 2 * e_loc * ff)
        gu[mb] = lax.dot_general(a, b, TN, preferred_element_type=F32)
        for cp in wide_copies(mb):
            cp.start()

        after(mb, 0, lambda: gather_dg.relay_minor(local.at[2]))
        after(mb, 2, gather_dg.share_own)
        after(mb, 3, scat_dh.turn)
        after(mb, 4, gather_dg.relay_major)
        after(mb, 5, gather_dg.share_near)
        return 0

    lax.fori_loop(0, n_m, wide_step, 0)

    n_blk = wd_s.shape[2]
    n_n = d // n_blk

    def down_copies(nb):
        slot = lax.rem(nb, 2)
        return [pltpu.make_async_copy(wd_s.at[slot, pl.ds(e * ff, ff)], dwd_hbm.at[e, :, rows(nb * n_blk, n_blk)], out_sem.at[n_m + slot, e]) for e in range(e_loc)]

    def down_step(nb, _):
        @pl.when(nb > 1)
        def _():
            for cp in down_copies(nb - 2):
                cp.wait()
        a = gated[...].reshape(n_tile * tile_rows, e_loc * ff)
        b = dys[:, :, rows(nb * n_blk, n_blk)].reshape(n_tile * tile_rows, n_blk)
        wd_s[lax.rem(nb, 2)] = lax.dot_general(a, b, TN, preferred_element_type=F32)
        for cp in down_copies(nb):
            cp.start()

        return 0

    early = n_n // 3
    lax.fori_loop(0, early, down_step, 0)
    scat_dh.relay_minor()
    gather_dg.share_far()

    for h in halves:
        r = pl.ds(h.which * blk, blk)
        y_ref[r] = (x_ref[r].astype(F32) + scat_y.total(h) + row_f32(bias_ref)).astype(BF16)

    gather_dg.wait(16, 17, 18, 19)
    for t in range(n_tile):
        which, tl = t // side, t % side
        pieces = []
        for ep in range(n_ep):
            px, pc = ep // CORES, ep % CORES
            total = None
            for py in range(side):
                if which == 0:
                    term = dgs[px, pl.ds((pc * side + py) * blk + tl * 8, 8)]
                else:
                    term = dgs[side + py, pl.ds((pc * side + px) * blk + tl * 8, 8)]
                total = term if total is None else total + term
            pieces.append(total)
        d_g = jnp.concatenate(pieces, axis=0)
        g_t = lax.dot_general(sel_t[...], hid[t, :, pl.ds(d, 128)], NT, preferred_element_type=F32)
        d_l = (g_t * (d_g - jnp.sum(g_t * d_g, axis=0, keepdims=True))).astype(BF16)
        dl_s[t] = d_l

    gain = row_f32(gain_ref)
    gain_part = jnp.zeros((1, d), F32)
    for h in halves:
        r = pl.ds(h.which * blk, blk)
        routed = lax.dot_general(dl_s[h.tile(0), :, mine], w_rt[...], TN, preferred_element_type=F32)
        own = jnp.zeros((blk, d), F32)
        for q in range(side):
            own = own + jnp.where(h.n == q, routed[q * blk:(q + 1) * blk], 0.0)
        x_f32 = x_ref[r].astype(F32)
        inv_rms = lax.rsqrt(jnp.mean(x_f32 * x_f32, axis=1, keepdims=True) + EPS)
        normed = x_f32 * inv_rms
        dh = scat_dh.total(h) + own
        gain_part = gain_part + jnp.sum(dh * normed, axis=0, keepdims=True)
        d_norm = dh * gain
        dx_ref[r] = (dy_in[r].astype(F32) + inv_rms * (d_norm - normed * jnp.mean(d_norm * normed, axis=1, keepdims=True))).astype(BF16)

    def spread(buf, slot, peers, first):
        return [pltpu.make_async_remote_copy(src_ref=buf.at[slot], dst_ref=buf.at[slot], send_sem=ar_send.at[first + o], recv_sem=ar_recv.at[first + o], device_id=peer, device_id_type=MESH) for o, peer in enumerate(peers)]

    ar1[me_ep] = gain_part
    over_ep = spread(ar1, me_ep, ep_peers, 0)
    for cp in over_ep:
        cp.start()
    dr_s[...] = jnp.zeros_like(dr_s)
    for t in range(n_tile):
        dr_s[...] += jnp.dot(dl_s[t], hid[t, :, pl.ds(0, d)], preferred_element_type=F32)
    for cp in over_ep:
        cp.wait_recv()
    ar2[place.y] = jnp.sum(ar1[...], axis=0)
    over_tp = spread(ar2, place.y, tp_peers, n_ep - 1)
    for cp in over_tp:
        cp.start()
    d_router_t[...] = jnp.dot(one_hot(pick, F32), dr_s[...], preferred_element_type=F32, precision=lax.Precision.HIGHEST)
    lax.fori_loop(early, n_n, down_step, 0)
    for cp in over_tp:
        cp.wait_recv()
    d_gain[...] = jnp.sum(ar2[...], axis=0)

    for cp in over_ep + over_tp:
        cp.wait_send()
    for g in (gather_h, gather_dy, gather_dg):
        g.finish()
    for sc in (scat_y, scat_dh):
        sc.finish()
    for s in (steps - 2, steps - 1):
        swap_copy(s, 1, index_of(s)).wait_send()
    for mb in range(n_m):
        for cp in wide_copies(mb):
            cp.wait()
    for nb in (n_n - 2, n_n - 1):
        for cp in down_copies(nb):
            cp.wait()


def moe(mesh, dy, x_in, gain, bias, w_r, idx, w_gate, w_up, w_down):
    side = mesh.shape["tp"]
    n_tok, d = dy.shape
    e_loc, _, ff = w_gate.shape
    tile_rows = CORES * side * n_tok // 2
    span = tile_rows // CORES
    n_tile = 2 * side
    n_ep = side * CORES
    n_exp = n_ep * e_loc
    dx = d + 128
    vm = pl.BlockSpec(memory_space=pltpu.VMEM)
    hbm = pl.BlockSpec(memory_space=pl.ANY)
    blk = n_tok // 2
    n_g, n_s = 2 * Gather.COPIES, 2 * Scatter.COPIES
    n_peer = n_ep + side - 2
    return pl.pallas_call(
        functools.partial(moe_kernel, side, d, e_loc, ff, n_exp),
        out_shape=(
            jax.ShapeDtypeStruct((n_tok, d), BF16),
            jax.ShapeDtypeStruct((n_tok, d), BF16),
            jax.ShapeDtypeStruct((1, d), F32),
            jax.ShapeDtypeStruct((1, d), F32),
            jax.ShapeDtypeStruct((n_exp, d), F32),
            jax.ShapeDtypeStruct(w_gate.shape, F32),
            jax.ShapeDtypeStruct(w_up.shape, F32),
            jax.ShapeDtypeStruct(w_down.shape, F32),
        ),
        in_specs=[vm] * 6 + [hbm] * 3,
        out_specs=(vm, vm, vm, vm, vm, hbm, hbm, hbm),
        scratch_shapes=[
            pltpu.VMEM((n_tile, tile_rows, dx), BF16),
            pltpu.VMEM((n_tile, tile_rows, d), BF16),
            pltpu.VMEM((n_tile, tile_rows, tile_rows), F32),
            pltpu.VMEM((n_tok, tile_rows), F32),
            pltpu.VMEM((d, 2 * e_loc * ff), BF16),
            pltpu.VMEM((e_loc * ff, d), BF16),
            pltpu.VMEM((n_tile, tile_rows, e_loc * ff), BF16),
            pltpu.VMEM((n_tile, tile_rows, 2 * e_loc * ff), BF16),
            pltpu.VMEM((n_tile, span, d), BF16),
            pltpu.VMEM((n_tile, span, d), BF16),
            pltpu.VMEM((2, tile_rows, d), BF16),
            pltpu.VMEM((n_tile, span, d), BF16),
            pltpu.VMEM((2, 3 * span, d), BF16),
            pltpu.VMEM((2, 3 * span, d), BF16),
            pltpu.VMEM((2, 3 * blk, d), BF16),
            pltpu.VMEM((2, 3 * blk, d), BF16),
            pltpu.VMEM((n_tile, tile_rows, 2 * e_loc * ff), F32),
            pltpu.VMEM((tile_rows, e_loc * ff), F32),
            pltpu.VMEM((tile_rows, e_loc * ff), F32),
            pltpu.VMEM((2, e_loc * ff, 256), F32),
            pltpu.VMEM((n_tile, 1, d), F32),
            pltpu.VMEM((n_tile, n_ep * 8, tile_rows), BF16),
            pltpu.VMEM((n_ep * 8, d), F32),
            pltpu.VMEM((n_ep, 1, d), F32),
            pltpu.VMEM((side, 1, d), F32),
            pltpu.VMEM((n_tok, dx), BF16),
            pltpu.VMEM((128, e_loc * ff), BF16),
            pltpu.VMEM((n_ep * 8, 128), BF16),
            pltpu.VMEM((n_ep * 8, d), BF16),
            pltpu.SemaphoreType.DMA((3 * e_loc,)),
            pltpu.SemaphoreType.DMA((3, 2)),
            pltpu.SemaphoreType.DMA((3, n_g)),
            pltpu.SemaphoreType.DMA((3, n_g)),
            pltpu.SemaphoreType.DMA((2, n_s)),
            pltpu.SemaphoreType.DMA((2, n_s)),
            pltpu.SemaphoreType.DMA((2,)),
            pltpu.SemaphoreType.DMA((2, n_tile)),
            pltpu.SemaphoreType.REGULAR,
            pltpu.SemaphoreType.DMA((d // tile_rows + 2, 2 * e_loc)),
            pltpu.SemaphoreType.DMA((n_peer,)),
            pltpu.SemaphoreType.DMA((n_peer,)),
        ],
        compiler_params=pltpu.CompilerParams(collective_id=0, has_side_effects=True, vmem_limit_bytes=67043328),
        name="moe",
    )(dy, x_in, gain, bias, w_r, idx, w_gate, w_up, w_down)


def emit_kernel(*refs):
    n = len(refs) // 2
    for src, dst in zip(refs[:3], refs[n:n + 3]):
        dst[...] = src[...]

    @pl.when(pl.program_id(0) == 0)
    def _():
        for src, dst in zip(refs[3:n], refs[n + 3:]):
            dst[...] = src[...].reshape(dst.shape)


def emit(wide_a, wide_b, down, *small):
    e_loc, d, ff = wide_a.shape
    n = d // 256
    wide = pl.BlockSpec((e_loc, 256, ff), lambda i: (0, i, 0))
    deep = pl.BlockSpec((e_loc, ff, 256), lambda i: (0, 0, i))
    whole = lambda v: pl.BlockSpec(v.shape, lambda i: (0,) * len(v.shape))
    shapes = [jax.ShapeDtypeStruct(v.shape if v.shape[0] > 1 else (v.shape[1],), v.dtype) for v in small]
    return pl.pallas_call(
        emit_kernel,
        grid=(n,),
        out_shape=tuple(jax.ShapeDtypeStruct(v.shape, v.dtype) for v in (wide_a, wide_b, down)) + tuple(shapes),
        in_specs=[wide, wide, deep] + [whole(v) for v in small],
        out_specs=(wide, wide, deep) + tuple(whole(v) for v in shapes),
        name="emit",
    )(wide_a, wide_b, down, *small)


def solution(mesh):
    tok_spec = P(("dp", "ep", "tp"), None)
    wide_spec = P("ep", None, "tp")
    down_spec = P("ep", "tp", None)
    grad_wide = P(("dp", "ep"), None, "tp")
    grad_down = P(("dp", "ep"), "tp", None)
    side = mesh.shape["tp"]
    assert mesh.shape["ep"] == side * CORES

    def device_step(x_in, norm_gain, w_router, expert_idx, w_gate, w_up, w_down, out_bias, dy_out):
        y_out, dx_in, d_gain, d_bias, d_router_t, d_gate, d_up, d_down = moe(mesh, dy_out, x_in, norm_gain, out_bias, w_router.T, expert_idx, w_gate, w_up, w_down)
        d_gate, d_up, d_down, y_out, dx_in, d_gain, d_bias, d_router_t = emit(d_gate, d_up, d_down, y_out, dx_in, d_gain, d_bias, d_router_t)
        return y_out, dx_in, d_gain, d_router_t.T, d_gate, d_up, d_down, d_bias

    return jax.shard_map(device_step, mesh=mesh, in_specs=(tok_spec, P(None), P(None, None), tok_spec, wide_spec, wide_spec, down_spec, P(None), tok_spec), out_specs=(tok_spec, tok_spec, P("dp"), P("dp", None), grad_wide, grad_wide, grad_down, P("dp")), check_vma=False)
```
